32 devices in a mesh: dp: 4 (over y, x), table: 8 (over z, core).
Axes of the slice: x: 2, y: 2, z: 4, core: 2. Of those that a mesh axis runs over, the one named last changes fastest.
Arguments:
- ids: int32 [16384], P('dp'), may hold values from 0 to 511
- lengths: int32 [32, 8], P(('dp', 'table')), may hold values from 1 to 64, 320 in all within a row
- table: bfloat16 [512, 512], P(None, 'table'), may hold values from -6 to 6
- w_uvqk: bfloat16 [512, 2048], replicated, may hold values from -0.25 to 0.25
- w_out: bfloat16 [512, 512], replicated, may hold values from -0.25 to 0.25
- cotangent: bfloat16 [16384, 512], P(('dp', 'table')), may hold values from -6 to 6
Outputs:
- output: bfloat16 [16384, 512], P(('dp', 'table'))
- grad_table: float32 [512, 512], P('dp', 'table')
- grad_uvqk: float32 [512, 2048], P(('dp', 'table'))
- grad_out_t: float32 [512, 512], P(('dp', 'table'))
The draws below stay inside these ranges and needn't reach their ends.
Inputs may be any that keep to these rules, and one draw needn't show every extreme that they name: Each device's 8 histories have lengths summing to 320, the longest exactly 64.
All inputs are finite; a program needn't handle non-finite values.
Results may differ from the reference program's by a relative error of at most 0.017.
Values may be sent and summed in bfloat16 or wider, within the bound.
No kernel may reach another device: no remote copies, remote signals or barrier semaphores. Data moves between devices by JAX's collectives and lax.ppermute only.
A program may use at most 64 MiB of HBM per device.

```python
import math
import jax
import jax.numpy as jnp
import numpy as np
from jax import lax

D = 512
H = 8
DH = 64
MAXLEN = 64
NH = 8
HD = 512
ROWS = 16384
ITEMS = 512
DEVICES = 32


def set_ends(array, key, least, top_value):
    longest = array.shape.index(max(array.shape))
    spots = []
    for shift in (0, 1):
        where = [jax.random.randint(jax.random.fold_in(key, axis), (), 0, length) for axis, length in enumerate(array.shape)]
        where[longest] = (where[longest] + shift) % array.shape[longest]
        spots.append(tuple(where))
    return array.at[spots[0]].set(least).at[spots[1]].set(top_value)


def block_levels(key, extent, cuts, least, top_value):
    factor_of, own = 1.0, jax.random.fold_in(key, 6)
    for dim, shards_of in cuts:
        heights = jnp.exp(jax.random.uniform(jax.random.fold_in(own, dim), (shards_of,), jnp.float32, least / len(cuts), top_value / len(cuts)))
        factor_of = factor_of * jnp.repeat(heights, extent[dim] // shards_of).reshape([-1 if axis == dim else 1 for axis in range(len(extent))])
    return factor_of


def profile(count, total, bound, lean):
    loads = [(1 << 20) // math.isqrt(standing ** lean) + 1 for standing in range(2, count + 1)]
    spare, holding = total - bound - (count - 1), [1] * (count - 1)
    while spare > 0:
        movable = [i for i in range(count - 1) if holding[i] < bound]
        pool, remaining = sum([loads[i] for i in movable]), spare
        for i in movable:
            addition = min(bound - holding[i], max(1, remaining * loads[i] // pool), spare)
            holding[i] = holding[i] + addition
            spare = spare - addition
    return np.array([bound] + holding)


def uneven(own_key, amount, total, most, slope):
    if amount == 2:
        one = jax.random.randint(own_key, (), max(1, total - most), min(most, total - 1) + 1)
        return jnp.stack([one, total - one])
    sizes = jnp.asarray(profile(amount, total, most, slope), jnp.int32)
    twos = (amount - 1) // 2
    donor, sink = sizes[1:1 + 2 * twos:2], sizes[2:2 + 2 * twos:2]
    margin = jnp.minimum(donor - 1, most - sink)
    passed = jax.random.randint(jax.random.fold_in(own_key, 1), (twos,), 0, 1 << 20) % (margin + 1)
    sizes = sizes.at[1:1 + 2 * twos:2].set(donor - passed).at[2:2 + 2 * twos:2].set(sink + passed)
    return sizes[jax.random.permutation(jax.random.fold_in(own_key, 2), amount)]


def gaussian(stream_key, shape, scale, bound, cuts=(), held_as=jnp.bfloat16):
    result = jax.random.normal(stream_key, shape, jnp.float32) * scale
    if len(cuts) > 0:
        result = block_levels(stream_key, shape, cuts, -0.22, 0.18) * result
    return jnp.clip(result, min=-bound, max=bound).astype(held_as)


def setup_inputs(seed: int = 0) -> dict:
    keys = jax.random.split(jax.random.key(seed), 7)
    ids = set_ends(jax.random.randint(keys[0], (ROWS,), 0, ITEMS), jax.random.fold_in(keys[0], 1), 0, ITEMS - 1).astype(jnp.int32)
    lengths = jax.vmap(lambda own: uneven(own, NH, NH * MAXLEN * 5 // 8, MAXLEN, 2))(jax.random.split(keys[1], DEVICES)).reshape((DEVICES, NH)).astype(jnp.int32)
    table = gaussian(keys[2], (ITEMS, D), 1.0, 6.0, ((1, 8),))
    w_uvqk = gaussian(keys[3], (D, 4 * HD), D ** -0.5, 0.25)
    w_out = gaussian(keys[4], (HD, D), HD ** -0.5, 0.25)
    cotangent = gaussian(keys[5], (ROWS, D), 1.0, 6.0, ((0, 32),))
    return dict(ids=ids, lengths=lengths, table=table, w_uvqk=w_uvqk, w_out=w_out, cotangent=cotangent)


eps_norm = 1e-05
block_histories = 64

def layer_norm(values):
    centre_mean = lax.optimization_barrier(jnp.mean(values, axis=-1, keepdims=True))
    centred = values - centre_mean
    spread = lax.optimization_barrier(jnp.mean(centred * centred, axis=-1, keepdims=True))
    return centred * lax.rsqrt(spread + eps_norm)

def front(inputs):
    return layer_norm(inputs).astype(jnp.bfloat16)

def middle(project, hist_len):
    histories, history_len, total_width = project.shape
    inner_width = total_width // 4
    activated = jax.nn.silu(project).astype(jnp.bfloat16)
    gate_heads = activated[..., :inner_width]
    value_heads = activated[..., inner_width:2 * inner_width].reshape(histories, history_len, H, DH)
    query_heads = activated[..., 2 * inner_width:3 * inner_width].reshape(histories, history_len, H, DH)
    key_heads = activated[..., 3 * inner_width:].reshape(histories, history_len, H, DH)
    scores = jnp.einsum('bihd,bjhd->bihj', query_heads.astype(jnp.float32), key_heads.astype(jnp.float32)) * DH ** (-0.5)
    position = jnp.arange(history_len, dtype=jnp.int32)
    allowed = (position[None, :, None, None] >= position[None, None, None, :]) & (position[None, :, None, None] < hist_len[:, None, None, None])
    weights = (jnp.where(allowed, jax.nn.silu(scores), jnp.zeros((), jnp.float32)) / MAXLEN).astype(jnp.bfloat16)
    attended = jnp.einsum('bihj,bjhd->bihd', weights.astype(jnp.float32), value_heads.astype(jnp.float32))
    attended = attended.reshape(histories, history_len, inner_width)
    return (layer_norm(attended) * gate_heads.astype(jnp.float32)).astype(jnp.bfloat16)

def layer_block(x_block, cot_block, hist_len, w_uvqk, w_out):
    histories, history_len, model_width = x_block.shape
    row_count = histories * history_len
    inputs = x_block.reshape(row_count, model_width).astype(jnp.float32)
    normed, front_back = jax.vjp(front, inputs)
    project = jnp.dot(normed, w_uvqk, preferred_element_type=jnp.float32)

    def middle_flat(flat_project):
        return middle(flat_project.reshape(histories, history_len, -1), hist_len).reshape(row_count, -1)
    gated_out, middle_back = jax.vjp(middle_flat, project)
    output = (inputs + jnp.dot(gated_out, w_out, preferred_element_type=jnp.float32)).astype(jnp.bfloat16)
    live_rows = (jnp.arange(history_len, dtype=jnp.int32)[None, :] < hist_len[:, None]).reshape(row_count, 1)
    out_grad = jnp.where(live_rows, cot_block.reshape(row_count, model_width), jnp.zeros((), jnp.bfloat16))
    grad_out_t = lax.dot_general(out_grad, gated_out, (((0,), (0,)), ((), ())), preferred_element_type=jnp.float32)
    gated_grad = lax.dot_general(out_grad, w_out, (((1,), (1,)), ((), ())), preferred_element_type=jnp.float32).astype(jnp.bfloat16)
    project_grad, = middle_back(gated_grad)
    project_grad_b = project_grad.astype(jnp.bfloat16)
    grad_uvqk = lax.dot_general(normed, project_grad_b, (((0,), (0,)), ((), ())), preferred_element_type=jnp.float32)
    normed_grad = lax.dot_general(project_grad_b, w_uvqk, (((1,), (1,)), ((), ())), preferred_element_type=jnp.float32).astype(jnp.bfloat16)
    front_grad, = front_back(normed_grad)
    input_grad = (front_grad + out_grad.astype(jnp.float32)).astype(jnp.bfloat16)
    return (output.reshape(histories, history_len, model_width), input_grad.reshape(histories, history_len, model_width), grad_uvqk, grad_out_t)

def reference(ids, lengths, table, w_uvqk, w_out, cotangent):
    embedded = jnp.take(table, ids, axis=0)
    histories = embedded.reshape(-1, MAXLEN, D)
    cot_hist = cotangent.reshape(-1, MAXLEN, D)
    flat_len = lengths.reshape(-1)
    total_hist = histories.shape[0]
    block_size = min(block_histories, total_hist)
    blocks = total_hist // block_size

    def scan_step(totals, pieces):
        x_block, cot_block, len_block = pieces
        out_block, grad_block, grad_u, grad_o = layer_block(x_block, cot_block, len_block, w_uvqk, w_out)
        return ((totals[0] + grad_u, totals[1] + grad_o), (out_block, grad_block))
    start_totals = (jnp.zeros(w_uvqk.shape, jnp.float32), jnp.zeros((w_out.shape[1], w_out.shape[0]), jnp.float32))
    stacked = (histories.reshape(blocks, block_size, MAXLEN, D), cot_hist.reshape(blocks, block_size, MAXLEN, D), flat_len.reshape(blocks, block_size))
    totals, results = lax.scan(scan_step, start_totals, stacked)
    output = results[0].reshape(-1, D)
    input_grad = results[1].reshape(-1, D)
    grad_table = jax.ops.segment_sum(input_grad.astype(jnp.float32), ids, num_segments=ITEMS)
    return (output, grad_table, totals[0], totals[1])
```

```python
import functools
import jax
import jax.numpy as jnp
from jax import lax
from jax.experimental import pallas as pl
from jax.experimental.pallas import tpu as pltpu
from jax.sharding import PartitionSpec as P

H = 8
DH = 64
MAXLEN = 64
LANES = 128
EPS = 1e-05
BF = jnp.bfloat16
F32 = jnp.float32


def nt(a, b):
    return lax.dot_general(a, b, (((1,), (1,)), ((), ())), preferred_element_type=F32)


def nn(a, b):
    return jnp.dot(a, b, preferred_element_type=F32)


def tn(a, b):
    return lax.dot_general(a, b, (((0,), (0,)), ((), ())), preferred_element_type=F32)


def sigmoid(v):
    return 0.5 * jnp.tanh(0.5 * v) + 0.5


def origin_of(packed, len_ref, histories):
    shift = jnp.zeros_like(packed)
    end = jnp.int32(0)
    for b in range(histories):
        end = end + len_ref[0, b]
        shift = shift + jnp.where(packed >= end, MAXLEN - len_ref[0, b], 0)
    return packed + shift


def start_of(packed, len_ref, histories):
    start = jnp.zeros_like(packed)
    end = jnp.int32(0)
    for b in range(histories):
        end = end + len_ref[0, b]
        start = jnp.where(packed >= end, end, start)
    return start


def prep_kernel(len_ref, ids_ref, cot_ref, wout_ref, onehot_ref, outg_ref, gg_ref):
    histories = len_ref.shape[1]
    live, items = onehot_ref.shape
    rows = ids_ref.shape[1]
    own = lax.axis_index("table")
    ids = ids_ref[pl.ds(own, 1), :].astype(F32)
    packed = lax.broadcasted_iota(jnp.int32, (live, rows), 0)
    take = origin_of(packed, len_ref, histories) == lax.broadcasted_iota(jnp.int32, (live, rows), 1)
    own_id = jnp.sum(jnp.where(take, ids, 0.0), axis=1, keepdims=True).astype(jnp.int32)
    onehot_ref[...] = jnp.where(
        lax.broadcasted_iota(jnp.int32, (live, items), 1) == own_id, 1.0, 0.0
    ).astype(BF)
    out_grad = nn(jnp.where(take, 1.0, 0.0).astype(BF), cot_ref[...]).astype(BF)
    outg_ref[...] = out_grad
    gg_ref[...] = nt(out_grad, wout_ref[...]).astype(BF)


def out_kernel(len_ref, ids_ref, tab_ref, gated_ref, wout_ref, out_ref):
    histories = len_ref.shape[1]
    rows = ids_ref.shape[1]
    live = gated_ref.shape[0]
    items = tab_ref.shape[1]
    own = lax.axis_index("table")
    ids = ids_ref[pl.ds(own, 1), :].astype(F32)
    ids_col = jnp.transpose(jnp.broadcast_to(ids, (LANES, rows))).astype(jnp.int32)
    lane = lax.broadcasted_iota(jnp.int32, (rows, LANES), 1)
    onehot = jnp.concatenate(
        [jnp.where(ids_col == lane + k, 1.0, 0.0).astype(BF) for k in range(0, items, LANES)], axis=1
    )
    packed = lax.broadcasted_iota(jnp.int32, (rows, live), 1)
    put = origin_of(packed, len_ref, histories) == lax.broadcasted_iota(jnp.int32, (rows, live), 0)
    gated = nn(jnp.where(put, 1.0, 0.0).astype(BF), gated_ref[...]).astype(BF)
    out_ref[...] = (nt(onehot, tab_ref[...]) + nn(gated, wout_ref[...])).astype(BF)


def layer_kernel(
    order, shape, len_ref, tab_ref, onehot_ref, outg_ref, gg_ref, w_ref, gated_ref, *refs
):
    grads, scratch = refs[:-9], refs[-9:]
    layer_body(order, shape, len_ref, tab_ref, onehot_ref, outg_ref, gg_ref, w_ref, gated_ref, grads, *scratch)


def layer_body(
    order, shape, len_ref, tab_ref, onehot_ref, outg_ref, gg_ref, w_ref, gated_ref, grads,
    act_ref, dact_ref, fac_ref, att_ref, attended_ref, dkv_ref, pg_ref, tmp_ref, lhs_ref,
):
    histories = len_ref.shape[1]
    live, items = onehot_ref.shape
    width = tab_ref.shape[0]
    dps, tabs = shape
    devices = dps * tabs
    me_dp = lax.axis_index("dp")
    me_tab = lax.axis_index("table")
    me = me_dp * tabs + me_tab
    blk = width // devices
    half = width // 2

    x = nt(onehot_ref[...], tab_ref[...])
    centred = x - jnp.mean(x, axis=1, keepdims=True)
    rstd = lax.rsqrt(jnp.mean(centred * centred, axis=1, keepdims=True) + EPS)
    xhat = centred * rstd
    normed = xhat.astype(BF)
    for g in range(4):
        cols = slice(g * width, (g + 1) * width)
        p = nn(normed, w_ref[:, cols])
        s = sigmoid(p)
        a = p * s
        act_ref[:, cols] = a.astype(BF)
        dact_ref[:, cols] = s + a * (1.0 - s)

    tiles = live // MAXLEN
    pairs = width // LANES
    low = lax.broadcasted_iota(jnp.int32, (MAXLEN, LANES), 1) < DH
    zero = jnp.zeros((MAXLEN, LANES), BF)

    def stack(v):
        return jnp.concatenate([jnp.where(low, v, zero), jnp.where(low, zero, v)], axis=0)

    def merge(v):
        return jnp.where(low, v[:MAXLEN], v[MAXLEN:])

    for t in range(tiles):
        r0 = t * MAXLEN
        w0 = max(t - 1, 0) * MAXLEN
        row = r0 + lax.broadcasted_iota(jnp.int32, (MAXLEN, LANES), 0)
        col = w0 + lax.broadcasted_iota(jnp.int32, (MAXLEN, LANES), 1)
        seen = (col >= start_of(row, len_ref, histories)) & (col <= row)
        mask = jnp.where(seen, 1.0 / MAXLEN, 0.0)
        mask = jnp.concatenate([mask, mask], axis=0)
        for c in range(pairs):
            lo, hi = c * LANES, (c + 1) * LANES
            q = stack(act_ref[r0 : r0 + MAXLEN, 2 * width + lo : 2 * width + hi])
            k = act_ref[w0 : w0 + LANES, 3 * width + lo : 3 * width + hi]
            v = act_ref[w0 : w0 + LANES, width + lo : width + hi]
            sc = nt(q, k) * DH**-0.5
            sg = sigmoid(sc)
            si = sc * sg
            w = (si * mask).astype(BF)
            fac_ref[t * pairs + c] = (sg + si * (1.0 - sg)) * (mask * DH**-0.5)
            att_ref[t * pairs + c] = w
            attended_ref[r0 : r0 + MAXLEN, lo:hi] = merge(nn(w, v))

    attended = attended_ref[...]
    cen = attended - jnp.mean(attended, axis=1, keepdims=True)
    r = lax.rsqrt(jnp.mean(cen * cen, axis=1, keepdims=True) + EPS)
    yhat = cen * r
    u = act_ref[:, :width].astype(F32)
    gated = (yhat * u).astype(BF)
    gated_ref[...] = gated
    gg = gg_ref[...].astype(F32)
    pg_ref[:, :width] = ((gg * yhat).astype(BF).astype(F32) * dact_ref[:, :width]).astype(BF)
    dy = gg * u
    datt = r * (dy - jnp.mean(dy, axis=1, keepdims=True) - yhat * jnp.mean(dy * yhat, axis=1, keepdims=True))
    attended_ref[...] = datt

    dkv_ref[...] = jnp.zeros_like(dkv_ref)
    for t in range(tiles):
        r0 = t * MAXLEN
        w0 = max(t - 1, 0) * MAXLEN
        for c in range(pairs):
            lo, hi = c * LANES, (c + 1) * LANES
            q = stack(act_ref[r0 : r0 + MAXLEN, 2 * width + lo : 2 * width + hi])
            k = act_ref[w0 : w0 + LANES, 3 * width + lo : 3 * width + hi]
            v = act_ref[w0 : w0 + LANES, width + lo : width + hi]
            da = stack(attended_ref[r0 : r0 + MAXLEN, lo:hi].astype(BF))
            dw = nt(da, v).astype(BF).astype(F32)
            ds = (dw * fac_ref[t * pairs + c]).astype(BF)
            dq = merge(nn(ds, k)).astype(BF).astype(F32)
            qc = slice(2 * width + lo, 2 * width + hi)
            pg_ref[r0 : r0 + MAXLEN, qc] = (dq * dact_ref[r0 : r0 + MAXLEN, qc]).astype(BF)
            dkv_ref[w0 : w0 + LANES, lo:hi] += tn(att_ref[t * pairs + c], da)
            dkv_ref[w0 : w0 + LANES, width + lo : width + hi] += tn(ds, q)
    for g, c in ((1, 0), (3, 1)):
        cols = slice(g * width, (g + 1) * width)
        d = dkv_ref[:, c * width : (c + 1) * width].astype(BF).astype(F32)
        pg_ref[:, cols] = (d * dact_ref[:, cols]).astype(BF)

    dn = nt(pg_ref[...], w_ref[...]).astype(BF).astype(F32)
    dx = rstd * (dn - jnp.mean(dn, axis=1, keepdims=True) - xhat * jnp.mean(dn * xhat, axis=1, keepdims=True))
    in_grad = (dx + outg_ref[...].astype(F32)).astype(BF)

    def position(colour, rel):
        place = 0
        for bit in order[colour]:
            place = place * 2 + ((rel >> bit) & 1)
        return place

    def relative(colour, src):
        tmp_ref[...] = src
        for rel in range(devices):
            at = position(colour, rel) * blk
            src_at = pl.multiple_of((me ^ rel) * blk, blk)
            lhs_ref[at : at + blk, :] = tmp_ref[pl.ds(src_at, blk), :]
        return lhs_ref[...]

    normed_t = jnp.transpose(normed)
    outg_t = jnp.transpose(outg_ref[...])
    if order is None:
        grad_o_ref, grad_u_ref, grad_t_ref = grads
        grad_o_ref[...] = nn(outg_t, gated)
        grad_u_ref[...] = nn(normed_t, pg_ref[...])
        grad_t_ref[...] = nn(jnp.transpose(in_grad), onehot_ref[...]).astype(BF)
        return
    keep1_ref, send1_ref, keep2_ref, send2_ref = grads
    lhs = relative(0, outg_t)
    res = nn(lhs, gated).astype(BF)
    keep1_ref[:, :width] = res[:half]
    send1_ref[:, :width] = res[half:]
    lhs = relative(0, normed_t)
    res = nn(lhs, pg_ref[:, : 2 * width]).astype(BF)
    keep1_ref[:, width:] = res[:half]
    send1_ref[:, width:] = res[half:]
    lhs = relative(1, normed_t)
    res = nn(lhs, pg_ref[:, 2 * width :]).astype(BF)
    keep2_ref[:, : 2 * width] = res[:half]
    send2_ref[:, : 2 * width] = res[half:]
    tmp_ref[...] = jnp.transpose(in_grad)
    feats = width // tabs
    span = items // dps
    for rt in range(tabs):
        at = pl.multiple_of((me_tab ^ rt) * feats, feats)
        lhs_ref[rt * feats : (rt + 1) * feats, :] = tmp_ref[pl.ds(at, feats), :]
    for rd in range(dps):
        at = pl.multiple_of((me_dp ^ rd) * span, span)
        res = nn(lhs_ref[...], onehot_ref[:, pl.ds(at, span)]).astype(BF)
        for rt in range(tabs):
            place = position(1, rd * tabs + rt) * blk
            dst = keep2_ref if place < half else send2_ref
            place = place % half
            for j in range(feats // blk):
                dst[place : place + blk, 2 * width + j * span : 2 * width + (j + 1) * span] = res[
                    rt * feats + j * blk : rt * feats + (j + 1) * blk, :
                ]


VMEM_SPEC = pl.BlockSpec(memory_space=pltpu.VMEM)
SMEM_SPEC = pl.BlockSpec(memory_space=pltpu.SMEM)


def swap(v, bit, tab_bits, dps, tabs):
    if bit < tab_bits:
        return lax.ppermute(v, "table", [(i, i ^ (1 << bit)) for i in range(tabs)])
    b = bit - tab_bits
    return lax.ppermute(v, "dp", [(i, i ^ (1 << b)) for i in range(dps)])


def local(ids, lengths, table, w_uvqk, w_out, cotangent):
    tabs = lax.axis_size("table")
    dps = lax.axis_size("dp")
    devices = tabs * dps
    tab_bits = tabs.bit_length() - 1
    bits = devices.bit_length() - 1
    histories = lengths.shape[1]
    rows = histories * MAXLEN
    live = rows * 5 // 8
    items = table.shape[0]
    feats = table.shape[1]
    width = feats * tabs
    ids2 = ids.reshape(tabs, rows)

    onehot, outg, gg = pl.pallas_call(
        prep_kernel,
        out_shape=(
            jax.ShapeDtypeStruct((live, items), BF),
            jax.ShapeDtypeStruct((live, width), BF),
            jax.ShapeDtypeStruct((live, width), BF),
        ),
        in_specs=[SMEM_SPEC, VMEM_SPEC, VMEM_SPEC, VMEM_SPEC],
        out_specs=(VMEM_SPEC,) * 3,
        name="prep",
    )(lengths, ids2, cotangent, w_out)

    tab_t = lax.all_gather(table.T, "table", axis=0, tiled=True)

    dp_order = list(range(tab_bits, bits))
    z_order = list(range(1, tab_bits))
    order = ([0] + dp_order + z_order, [0] + dp_order[::-1] + z_order)
    w1 = 3 * width
    sds = jax.ShapeDtypeStruct
    blk = width // devices
    span = items // dps
    halving = blk % 16 == 0 and feats % blk == 0 and span == LANES and width % (feats // blk * span) == 0
    if halving:
        grad_shapes = (sds((width // 2, w1), BF),) * 4
    else:
        order = None
        grad_shapes = (sds((width, width), F32), sds((width, 4 * width), F32), sds((width, items), BF))
    tiles = live // MAXLEN * (width // LANES)
    gated, *grads = pl.pallas_call(
        functools.partial(layer_kernel, order, (dps, tabs)),
        out_shape=(sds((live, width), BF),) + grad_shapes,
        in_specs=[SMEM_SPEC] + [VMEM_SPEC] * 5,
        out_specs=(VMEM_SPEC,) * (1 + len(grad_shapes)),
        scratch_shapes=[
            pltpu.VMEM((live, 4 * width), BF),
            pltpu.VMEM((live, 4 * width), F32),
            pltpu.VMEM((tiles, LANES, LANES), F32),
            pltpu.VMEM((tiles, LANES, LANES), BF),
            pltpu.VMEM((live, width), F32),
            pltpu.VMEM((live, 2 * width), F32),
            pltpu.VMEM((live, 4 * width), BF),
            pltpu.VMEM((width, live), BF),
            pltpu.VMEM((width, live), BF),
        ],
        name="layer",
    )(lengths, tab_t, onehot, outg, gg, w_uvqk)

    output = pl.pallas_call(
        out_kernel,
        out_shape=sds((rows, width), BF),
        in_specs=[SMEM_SPEC] + [VMEM_SPEC] * 4,
        out_specs=VMEM_SPEC,
        name="out",
    )(lengths, ids2, tab_t, gated, w_out)

    if not halving:
        grad_o, grad_u, grad_t = grads
        grad_t = grad_t.reshape(tabs, feats, dps, span).transpose(2, 0, 1, 3).reshape(devices, feats * span)

        def share(v):
            v = lax.psum_scatter(v, "dp", scatter_dimension=0, tiled=True)
            return lax.psum_scatter(v, "table", scatter_dimension=0, tiled=True)

        return (output, share(grad_t).astype(F32).reshape(feats, span).T, share(grad_u), share(grad_o))

    keep1, send1, keep2, send2 = grads
    parts = []
    for keep, send, bit_order in ((keep1, send1, order[0]), (keep2, send2, order[1])):
        for n, bit in enumerate(bit_order):
            got = swap(send, bit, tab_bits, dps, tabs)
            total = keep.astype(F32) + got.astype(F32)
            if n + 1 < len(bit_order):
                total = total.astype(BF)
                h = total.shape[0] // 2
                keep, send = total[:h], total[h:]
        parts.append(total)
    one, two = parts
    grad_out_t = one[:, :width]
    grad_uvqk = jnp.concatenate([one[:, width:], two[:, : 2 * width]], axis=1)
    gt = jnp.concatenate([two[:, 2 * width + j * span : 2 * width + (j + 1) * span] for j in range(feats // blk)], axis=0)
    return (output, gt.T, grad_uvqk, grad_out_t)


def solution(mesh):
    return jax.shard_map(
        local,
        mesh=mesh,
        in_specs=(
            P("dp"),
            P(("dp", "table"), None),
            P(None, "table"),
            P(),
            P(),
            P(("dp", "table"), None),
        ),
        out_specs=(
            P(("dp", "table"), None),
            P("dp", "table"),
            P(("dp", "table"), None),
            P(("dp", "table"), None),
        ),
        check_vma=False,
    )
```

```python
import functools
import jax
import jax.numpy as jnp
from jax import lax
from jax.experimental import pallas as pl
from jax.experimental.pallas import tpu as pltpu
from jax.sharding import PartitionSpec as P

H = 8
DH = 64
MAXLEN = 64
LANES = 128
EPS = 1e-05
BF = jnp.bfloat16
F32 = jnp.float32


def nt(a, b):
    return lax.dot_general(a, b, (((1,), (1,)), ((), ())), preferred_element_type=F32)


def nn(a, b):
    return jnp.dot(a, b, preferred_element_type=F32)


def tn(a, b):
    return lax.dot_general(a, b, (((0,), (0,)), ((), ())), preferred_element_type=F32)


def sigmoid(v):
    return 0.5 * jnp.tanh(0.5 * v) + 0.5


def origin_of(packed, len_ref, histories):
    shift = jnp.zeros_like(packed)
    end = jnp.int32(0)
    for b in range(histories):
        end = end + len_ref[0, b]
        shift = shift + jnp.where(packed >= end, MAXLEN - len_ref[0, b], 0)
    return packed + shift


def start_of(packed, len_ref, histories):
    start = jnp.zeros_like(packed)
    end = jnp.int32(0)
    for b in range(histories):
        end = end + len_ref[0, b]
        start = jnp.where(packed >= end, end, start)
    return start


def prep_kernel(len_ref, ids_ref, cot_ref, wout_ref, onehot_ref, outg_ref, gg_ref):
    histories = len_ref.shape[1]
    live, items = onehot_ref.shape
    rows = ids_ref.shape[1]
    own = lax.axis_index("table")
    ids = ids_ref[pl.ds(own, 1), :].astype(F32)
    packed = lax.broadcasted_iota(jnp.int32, (live, rows), 0)
    take = origin_of(packed, len_ref, histories) == lax.broadcasted_iota(jnp.int32, (live, rows), 1)
    own_id = jnp.sum(jnp.where(take, ids, 0.0), axis=1, keepdims=True).astype(jnp.int32)
    onehot_ref[...] = jnp.where(
        lax.broadcasted_iota(jnp.int32, (live, items), 1) == own_id, 1.0, 0.0
    ).astype(BF)
    out_grad = nn(jnp.where(take, 1.0, 0.0).astype(BF), cot_ref[...]).astype(BF)
    outg_ref[...] = out_grad
    gg_ref[...] = nt(out_grad, wout_ref[...]).astype(BF)


def out_kernel(len_ref, ids_ref, tab_ref, gated_ref, wout_ref, out_ref):
    histories = len_ref.shape[1]
    rows = ids_ref.shape[1]
    live = gated_ref.shape[0]
    items = tab_ref.shape[1]
    own = lax.axis_index("table")
    ids = ids_ref[pl.ds(own, 1), :].astype(F32)
    ids_col = jnp.transpose(jnp.broadcast_to(ids, (LANES, rows))).astype(jnp.int32)
    lane = lax.broadcasted_iota(jnp.int32, (rows, LANES), 1)
    onehot = jnp.concatenate(
        [jnp.where(ids_col == lane + k, 1.0, 0.0).astype(BF) for k in range(0, items, LANES)], axis=1
    )
    packed = lax.broadcasted_iota(jnp.int32, (rows, live), 1)
    put = origin_of(packed, len_ref, histories) == lax.broadcasted_iota(jnp.int32, (rows, live), 0)
    gated = nn(jnp.where(put, 1.0, 0.0).astype(BF), gated_ref[...]).astype(BF)
    out_ref[...] = (nt(onehot, tab_ref[...]) + nn(gated, wout_ref[...])).astype(BF)


def layer_kernel(order, shape, len_ref, onehot_ref, outg_ref, gg_ref, w_ref, *refs):
    dps, tabs = shape
    pieces, refs = refs[:tabs], refs[tabs:]
    gated_ref, tab_ref = refs[:2]
    grads, scratch = refs[2:-9], refs[-9:]
    me_tab = lax.axis_index("table")
    for rel in range(tabs):
        feats = pieces[rel].shape[0]
        at = pl.multiple_of((me_tab ^ rel) * feats, feats)
        tab_ref[pl.ds(at, feats), :] = pieces[rel][...]
    layer_body(order, shape, len_ref, tab_ref, onehot_ref, outg_ref, gg_ref, w_ref, gated_ref, grads, *scratch)


def layer_body(
    order, shape, len_ref, tab_ref, onehot_ref, outg_ref, gg_ref, w_ref, gated_ref, grads,
    act_ref, dact_ref, fac_ref, att_ref, attended_ref, dkv_ref, pg_ref, tmp_ref, lhs_ref,
):
    histories = len_ref.shape[1]
    live, items = onehot_ref.shape
    width = tab_ref.shape[0]
    dps, tabs = shape
    devices = dps * tabs
    me_dp = lax.axis_index("dp")
    me_tab = lax.axis_index("table")
    me = me_dp * tabs + me_tab
    blk = width // devices
    half = width // 2

    x = nt(onehot_ref[...], tab_ref[...])
    centred = x - jnp.mean(x, axis=1, keepdims=True)
    rstd = lax.rsqrt(jnp.mean(centred * centred, axis=1, keepdims=True) + EPS)
    xhat = centred * rstd
    normed = xhat.astype(BF)
    for g in range(4):
        cols = slice(g * width, (g + 1) * width)
        p = nn(normed, w_ref[:, cols])
        s = sigmoid(p)
        a = p * s
        act_ref[:, cols] = a.astype(BF)
        dact_ref[:, cols] = s + a * (1.0 - s)

    tiles = live // MAXLEN
    pairs = width // LANES
    low = lax.broadcasted_iota(jnp.int32, (MAXLEN, LANES), 1) < DH
    zero = jnp.zeros((MAXLEN, LANES), BF)

    def stack(v):
        return jnp.concatenate([jnp.where(low, v, zero), jnp.where(low, zero, v)], axis=0)

    def merge(v):
        return jnp.where(low, v[:MAXLEN], v[MAXLEN:])

    for t in range(tiles):
        r0 = t * MAXLEN
        w0 = max(t - 1, 0) * MAXLEN
        row = r0 + lax.broadcasted_iota(jnp.int32, (MAXLEN, LANES), 0)
        col = w0 + lax.broadcasted_iota(jnp.int32, (MAXLEN, LANES), 1)
        seen = (col >= start_of(row, len_ref, histories)) & (col <= row)
        mask = jnp.where(seen, 1.0 / MAXLEN, 0.0)
        mask = jnp.concatenate([mask, mask], axis=0)
        for c in range(pairs):
            lo, hi = c * LANES, (c + 1) * LANES
            q = stack(act_ref[r0 : r0 + MAXLEN, 2 * width + lo : 2 * width + hi])
            k = act_ref[w0 : w0 + LANES, 3 * width + lo : 3 * width + hi]
            v = act_ref[w0 : w0 + LANES, width + lo : width + hi]
            sc = nt(q, k) * DH**-0.5
            sg = sigmoid(sc)
            si = sc * sg
            w = (si * mask).astype(BF)
            fac_ref[t * pairs + c] = (sg + si * (1.0 - sg)) * (mask * DH**-0.5)
            att_ref[t * pairs + c] = w
            attended_ref[r0 : r0 + MAXLEN, lo:hi] = merge(nn(w, v))

    attended = attended_ref[...]
    cen = attended - jnp.mean(attended, axis=1, keepdims=True)
    r = lax.rsqrt(jnp.mean(cen * cen, axis=1, keepdims=True) + EPS)
    yhat = cen * r
    u = act_ref[:, :width].astype(F32)
    gated = (yhat * u).astype(BF)
    gated_ref[...] = gated
    gg = gg_ref[...].astype(F32)
    pg_ref[:, :width] = ((gg * yhat).astype(BF).astype(F32) * dact_ref[:, :width]).astype(BF)
    dy = gg * u
    datt = r * (dy - jnp.mean(dy, axis=1, keepdims=True) - yhat * jnp.mean(dy * yhat, axis=1, keepdims=True))
    attended_ref[...] = datt

    dkv_ref[...] = jnp.zeros_like(dkv_ref)
    for t in range(tiles):
        r0 = t * MAXLEN
        w0 = max(t - 1, 0) * MAXLEN
        for c in range(pairs):
            lo, hi = c * LANES, (c + 1) * LANES
            q = stack(act_ref[r0 : r0 + MAXLEN, 2 * width + lo : 2 * width + hi])
            k = act_ref[w0 : w0 + LANES, 3 * width + lo : 3 * width + hi]
            v = act_ref[w0 : w0 + LANES, width + lo : width + hi]
            da = stack(attended_ref[r0 : r0 + MAXLEN, lo:hi].astype(BF))
            dw = nt(da, v).astype(BF).astype(F32)
            ds = (dw * fac_ref[t * pairs + c]).astype(BF)
            dq = merge(nn(ds, k)).astype(BF).astype(F32)
            qc = slice(2 * width + lo, 2 * width + hi)
            pg_ref[r0 : r0 + MAXLEN, qc] = (dq * dact_ref[r0 : r0 + MAXLEN, qc]).astype(BF)
            dkv_ref[w0 : w0 + LANES, lo:hi] += tn(att_ref[t * pairs + c], da)
            dkv_ref[w0 : w0 + LANES, width + lo : width + hi] += tn(ds, q)
    for g, c in ((1, 0), (3, 1)):
        cols = slice(g * width, (g + 1) * width)
        d = dkv_ref[:, c * width : (c + 1) * width].astype(BF).astype(F32)
        pg_ref[:, cols] = (d * dact_ref[:, cols]).astype(BF)

    dn = nt(pg_ref[...], w_ref[...]).astype(BF).astype(F32)
    dx = rstd * (dn - jnp.mean(dn, axis=1, keepdims=True) - xhat * jnp.mean(dn * xhat, axis=1, keepdims=True))
    in_grad = (dx + outg_ref[...].astype(F32)).astype(BF)

    def position(colour, rel):
        place = 0
        for bit in order[colour]:
            place = place * 2 + ((rel >> bit) & 1)
        return place

    def relative(colour, src):
        tmp_ref[...] = src
        for rel in range(devices):
            at = position(colour, rel) * blk
            src_at = pl.multiple_of((me ^ rel) * blk, blk)
            lhs_ref[at : at + blk, :] = tmp_ref[pl.ds(src_at, blk), :]
        return lhs_ref[...]

    normed_t = jnp.transpose(normed)
    outg_t = jnp.transpose(outg_ref[...])
    if order is None:
        grad_o_ref, grad_u_ref, grad_t_ref = grads
        grad_o_ref[...] = nn(outg_t, gated)
        grad_u_ref[...] = nn(normed_t, pg_ref[...])
        grad_t_ref[...] = nn(jnp.transpose(in_grad), onehot_ref[...]).astype(BF)
        return
    keep1_ref, send1_ref, keep2_ref, send2_ref = grads
    lhs = relative(0, outg_t)
    res = nn(lhs, gated).astype(BF)
    keep1_ref[:, :width] = res[:half]
    send1_ref[:, :width] = res[half:]
    lhs = relative(0, normed_t)
    res = nn(lhs, pg_ref[:, : 2 * width]).astype(BF)
    keep1_ref[:, width:] = res[:half]
    send1_ref[:, width:] = res[half:]
    lhs = relative(1, normed_t)
    res = nn(lhs, pg_ref[:, 2 * width :]).astype(BF)
    keep2_ref[:, : 2 * width] = res[:half]
    send2_ref[:, : 2 * width] = res[half:]
    tmp_ref[...] = jnp.transpose(in_grad)
    feats = width // tabs
    span = items // dps
    for rt in range(tabs):
        at = pl.multiple_of((me_tab ^ rt) * feats, feats)
        lhs_ref[rt * feats : (rt + 1) * feats, :] = tmp_ref[pl.ds(at, feats), :]
    for rd in range(dps):
        at = pl.multiple_of((me_dp ^ rd) * span, span)
        res = nn(lhs_ref[...], onehot_ref[:, pl.ds(at, span)]).astype(BF)
        for rt in range(tabs):
            place = position(1, rd * tabs + rt) * blk
            dst = keep2_ref if place < half else send2_ref
            place = place % half
            for j in range(feats // blk):
                dst[place : place + blk, 2 * width + j * span : 2 * width + (j + 1) * span] = res[
                    rt * feats + j * blk : rt * feats + (j + 1) * blk, :
                ]


def finish_kernel(keep_ref, got_ref, grad_u_ref, grad_o_ref, grad_t_ref):
    blk, width = grad_o_ref.shape
    feats, span = grad_t_ref.shape
    total = keep_ref[...].astype(F32) + got_ref[...].astype(F32)
    grad_o_ref[...] = total[:, :width]
    grad_u_ref[...] = total[:, width : 5 * width]
    for j in range(feats // blk):
        grad_t_ref[j * blk : (j + 1) * blk, :] = total[:, 5 * width + j * span : 5 * width + (j + 1) * span]


VMEM_SPEC = pl.BlockSpec(memory_space=pltpu.VMEM)
SMEM_SPEC = pl.BlockSpec(memory_space=pltpu.SMEM)


def swap(v, bit, tab_bits, dps, tabs):
    if bit < tab_bits:
        return lax.ppermute(v, "table", [(i, i ^ (1 << bit)) for i in range(tabs)])
    b = bit - tab_bits
    return lax.ppermute(v, "dp", [(i, i ^ (1 << b)) for i in range(dps)])


def local(ids, lengths, table, w_uvqk, w_out, cotangent):
    tabs = lax.axis_size("table")
    dps = lax.axis_size("dp")
    devices = tabs * dps
    tab_bits = tabs.bit_length() - 1
    bits = devices.bit_length() - 1
    histories = lengths.shape[1]
    rows = histories * MAXLEN
    live = rows * 5 // 8
    items = table.shape[0]
    feats = table.shape[1]
    width = feats * tabs
    ids2 = ids.reshape(tabs, rows)

    onehot, outg, gg = pl.pallas_call(
        prep_kernel,
        out_shape=(
            jax.ShapeDtypeStruct((live, items), BF),
            jax.ShapeDtypeStruct((live, width), BF),
            jax.ShapeDtypeStruct((live, width), BF),
        ),
        in_specs=[SMEM_SPEC, VMEM_SPEC, VMEM_SPEC, VMEM_SPEC],
        out_specs=(VMEM_SPEC,) * 3,
        compiler_params=pltpu.CompilerParams(vmem_limit_bytes=16 << 20),
        name="prep",
    )(lengths, ids2, cotangent, w_out)

    def other(v, rel):
        return lax.ppermute(v, "table", [(i, i ^ rel) for i in range(tabs)])

    mine = table.T
    pieces = []
    for rel in range(0, tabs, 2):
        piece = other(mine, rel) if rel else mine
        pieces += [piece, other(piece, 1)]

    dp_order = list(range(tab_bits, bits))
    z_order = list(range(1, tab_bits))
    order = ([0] + dp_order + z_order, [0] + dp_order[::-1] + z_order)
    w1 = 3 * width
    sds = jax.ShapeDtypeStruct
    blk = width // devices
    span = items // dps
    halving = blk % 16 == 0 and feats % blk == 0 and span == LANES and width % (feats // blk * span) == 0
    if halving:
        grad_shapes = (sds((width // 2, w1), BF),) * 4
    else:
        order = None
        grad_shapes = (sds((width, width), F32), sds((width, 4 * width), F32), sds((width, items), BF))
    tiles = live // MAXLEN * (width // LANES)
    gated, tab_t, *grads = pl.pallas_call(
        functools.partial(layer_kernel, order, (dps, tabs)),
        out_shape=(sds((live, width), BF), sds((width, items), BF)) + grad_shapes,
        in_specs=[SMEM_SPEC] + [VMEM_SPEC] * (4 + tabs),
        out_specs=(VMEM_SPEC,) * (2 + len(grad_shapes)),
        scratch_shapes=[
            pltpu.VMEM((live, 4 * width), BF),
            pltpu.VMEM((live, 4 * width), F32),
            pltpu.VMEM((tiles, LANES, LANES), F32),
            pltpu.VMEM((tiles, LANES, LANES), BF),
            pltpu.VMEM((live, width), F32),
            pltpu.VMEM((live, 2 * width), F32),
            pltpu.VMEM((live, 4 * width), BF),
            pltpu.VMEM((width, live), BF),
            pltpu.VMEM((width, live), BF),
        ],
        compiler_params=pltpu.CompilerParams(vmem_limit_bytes=32 << 20),
        name="layer",
    )(lengths, onehot, outg, gg, w_uvqk, *pieces)

    def finish_output(gated):
        return pl.pallas_call(
            out_kernel,
            out_shape=sds((rows, width), BF),
            in_specs=[SMEM_SPEC] + [VMEM_SPEC] * 4,
            out_specs=VMEM_SPEC,
            compiler_params=pltpu.CompilerParams(vmem_limit_bytes=16 << 20),
        name="out",
        )(lengths, ids2, tab_t, gated, w_out)

    if not halving:
        grad_o, grad_u, grad_t = grads
        grad_t = grad_t.reshape(tabs, feats, dps, span).transpose(2, 0, 1, 3).reshape(devices, feats * span)

        def share(v):
            v = lax.psum_scatter(v, "dp", scatter_dimension=0, tiled=True)
            return lax.psum_scatter(v, "table", scatter_dimension=0, tiled=True)

        return (finish_output(gated), share(grad_t).astype(F32).reshape(feats, span).T, share(grad_u), share(grad_o))

    def add(keep, got):
        return (keep.astype(F32) + got.astype(F32)).astype(BF)

    def halves(v):
        h = v.shape[0] // 2
        return v[:h], v[h:]

    keep1, send1, keep2, send2 = grads
    totals = [add(keep, other(send, 1)) for keep, send in ((keep1, send1), (keep2, send2))]
    gated, *totals = lax.optimization_barrier((gated, *totals))
    output = finish_output(gated)
    for n in range(len(dp_order)):
        for c in range(2):
            keep, send = halves(totals[c])
            totals[c] = add(keep, swap(send, order[c][1 + n], tab_bits, dps, tabs))
        if n == 0:
            output, *totals = lax.optimization_barrier((output, *totals))
    total = jnp.concatenate(totals, axis=1)
    for bit in z_order[:-1]:
        keep, send = halves(total)
        total = add(keep, swap(send, bit, tab_bits, dps, tabs))
    keep, send = halves(total)
    got = swap(send, z_order[-1], tab_bits, dps, tabs)
    grad_uvqk, grad_out_t, grad_t = pl.pallas_call(
        finish_kernel,
        out_shape=(sds((blk, 4 * width), F32), sds((blk, width), F32), sds((feats, span), F32)),
        in_specs=[VMEM_SPEC] * 2,
        out_specs=(VMEM_SPEC,) * 3,
        compiler_params=pltpu.CompilerParams(vmem_limit_bytes=8 << 20),
        name="finish",
    )(keep, got)
    return (output, grad_t.T, grad_uvqk, grad_out_t)


def solution(mesh):
    return jax.shard_map(
        local,
        mesh=mesh,
        in_specs=(
            P("dp"),
            P(("dp", "table"), None),
            P(None, "table"),
            P(),
            P(),
            P(("dp", "table"), None),
        ),
        out_specs=(
            P(("dp", "table"), None),
            P("dp", "table"),
            P(("dp", "table"), None),
            P(("dp", "table"), None),
        ),
        check_vma=False,
    )
```

```python
import functools
import jax
import jax.numpy as jnp
from jax import lax
from jax.experimental import pallas as pl
from jax.experimental.pallas import tpu as pltpu
from jax.sharding import PartitionSpec as P


DH = 64
MAXLEN = 64
LANES = 128
EPS = 1e-05
BF = jnp.bfloat16
F32 = jnp.float32


def nt(a, b):
    return lax.dot_general(a, b, (((1,), (1,)), ((), ())), preferred_element_type=F32)


def nn(a, b):
    return jnp.dot(a, b, preferred_element_type=F32)


def tn(a, b):
    return lax.dot_general(a, b, (((0,), (0,)), ((), ())), preferred_element_type=F32)


def sigmoid(v):
    return 0.5 * jnp.tanh(0.5 * v) + 0.5


def origin_of(packed, len_ref, histories):
    shift = jnp.zeros_like(packed)
    end = jnp.int32(0)
    for b in range(histories):
        end = end + len_ref[0, b]
        shift = shift + jnp.where(packed >= end, MAXLEN - len_ref[0, b], 0)
    return packed + shift


def start_of(packed, len_ref, histories):
    start = jnp.zeros_like(packed)
    end = jnp.int32(0)
    for b in range(histories):
        end = end + len_ref[0, b]
        start = jnp.where(packed >= end, end, start)
    return start


def prep_kernel(
    len_hbm, ids_ref, cot_hbm, wout_hbm, w_hbm, mine_hbm,
    onehot_ref, outg_ref, gg_ref, start_ref, origin_ref, w_ref, mine_ref,
    len_ref, cot_ref, wout_ref, sems,
):
    moves = [
        pltpu.make_async_copy(src, dst, sems.at[n])
        for n, (src, dst) in enumerate(
            ((len_hbm, len_ref), (cot_hbm, cot_ref), (wout_hbm, wout_ref), (w_hbm, w_ref), (mine_hbm, mine_ref))
        )
    ]
    for move in moves:
        move.start()
    histories = len_ref.shape[1]
    live, items = onehot_ref.shape
    rows = ids_ref.shape[1]
    own = lax.axis_index("table")
    ids = ids_ref[pl.ds(own, 1), :].astype(F32)
    moves[0].wait()
    start_ref[...] = start_of(lax.broadcasted_iota(jnp.int32, start_ref.shape, 0), len_ref, histories)
    origin_ref[...] = origin_of(lax.broadcasted_iota(jnp.int32, origin_ref.shape, 1), len_ref, histories)
    packed = lax.broadcasted_iota(jnp.int32, (live, rows), 0)
    take = origin_of(packed, len_ref, histories) == lax.broadcasted_iota(jnp.int32, (live, rows), 1)
    own_id = jnp.sum(jnp.where(take, ids, 0.0), axis=1, keepdims=True).astype(jnp.int32)
    onehot_ref[...] = jnp.where(
        lax.broadcasted_iota(jnp.int32, (live, items), 1) == own_id, 1.0, 0.0
    ).astype(BF)
    moves[1].wait()
    out_grad = nn(jnp.where(take, 1.0, 0.0).astype(BF), cot_ref[...]).astype(BF)
    outg_ref[...] = out_grad
    moves[2].wait()
    gg_ref[...] = nt(out_grad, wout_ref[...]).astype(BF)
    moves[3].wait()
    moves[4].wait()


def out_kernel(origin_ref, ids_ref, tab_ref, gated_ref, wout_ref, out_ref):
    rows = ids_ref.shape[1]
    live = gated_ref.shape[0]
    items = tab_ref.shape[1]
    own = lax.axis_index("table")
    ids = ids_ref[pl.ds(own, 1), :].astype(F32)
    ids_col = jnp.transpose(jnp.broadcast_to(ids, (LANES, rows))).astype(jnp.int32)
    lane = lax.broadcasted_iota(jnp.int32, (rows, LANES), 1)
    onehot = jnp.concatenate(
        [jnp.where(ids_col == lane + k, 1.0, 0.0).astype(BF) for k in range(0, items, LANES)], axis=1
    )
    put = origin_ref[0:1, :] == lax.broadcasted_iota(jnp.int32, (rows, live), 0)
    gated = nn(jnp.where(put, 1.0, 0.0).astype(BF), gated_ref[...]).astype(BF)
    out_ref[...] = (nt(onehot, tab_ref[...]) + nn(gated, wout_ref[...])).astype(BF)


def layer_kernel(order, shape, start_ref, onehot_ref, outg_ref, gg_ref, w_ref, *refs):
    _, tabs = shape
    pieces, refs = refs[:tabs], refs[tabs:]
    gated_ref, tab_ref = refs[:2]
    grads, scratch = refs[2:-9], refs[-9:]
    me_tab = lax.axis_index("table")
    for rel in range(tabs):
        feats = pieces[rel].shape[0]
        at = pl.multiple_of((me_tab ^ rel) * feats, feats)
        tab_ref[pl.ds(at, feats), :] = pieces[rel][...]
    layer_body(order, shape, start_ref, tab_ref, onehot_ref, outg_ref, gg_ref, w_ref, gated_ref, grads, *scratch)


def layer_body(
    order, shape, start_ref, tab_ref, onehot_ref, outg_ref, gg_ref, w_ref, gated_ref, grads,
    act_ref, dact_ref, fac_ref, att_ref, attended_ref, dkv_ref, pg_ref, tmp_ref, lhs_ref,
):
    live, items = onehot_ref.shape
    width = tab_ref.shape[0]
    dps, tabs = shape
    devices = dps * tabs
    me_dp = lax.axis_index("dp")
    me_tab = lax.axis_index("table")
    me = me_dp * tabs + me_tab
    blk = width // devices
    half = width // 2

    x = nt(onehot_ref[...], tab_ref[...])
    centred = x - jnp.mean(x, axis=1, keepdims=True)
    rstd = lax.rsqrt(jnp.mean(centred * centred, axis=1, keepdims=True) + EPS)
    xhat = centred * rstd
    normed = xhat.astype(BF)
    for g in range(4):
        cols = slice(g * width, (g + 1) * width)
        p = nn(normed, w_ref[:, cols])
        s = sigmoid(p)
        a = p * s
        act_ref[:, cols] = a.astype(BF)
        dact_ref[:, cols] = s + a * (1.0 - s)

    tiles = live // MAXLEN
    pairs = width // LANES
    low = lax.broadcasted_iota(jnp.int32, (MAXLEN, LANES), 1) < DH
    zero = jnp.zeros((MAXLEN, LANES), BF)

    def stack(v):
        return jnp.concatenate([jnp.where(low, v, zero), jnp.where(low, zero, v)], axis=0)

    def merge(v):
        return jnp.where(low, v[:MAXLEN], v[MAXLEN:])

    for t in range(tiles):
        r0 = t * MAXLEN
        w0 = max(t - 1, 0) * MAXLEN
        row = r0 + lax.broadcasted_iota(jnp.int32, (MAXLEN, LANES), 0)
        col = w0 + lax.broadcasted_iota(jnp.int32, (MAXLEN, LANES), 1)
        seen = (col >= start_ref[r0 : r0 + MAXLEN, :]) & (col <= row)
        mask = jnp.where(seen, 1.0 / MAXLEN, 0.0)
        mask = jnp.concatenate([mask, mask], axis=0)
        for c in range(pairs):
            lo, hi = c * LANES, (c + 1) * LANES
            q = stack(act_ref[r0 : r0 + MAXLEN, 2 * width + lo : 2 * width + hi])
            k = act_ref[w0 : w0 + LANES, 3 * width + lo : 3 * width + hi]
            v = act_ref[w0 : w0 + LANES, width + lo : width + hi]
            sc = nt(q, k) * DH**-0.5
            sg = sigmoid(sc)
            si = sc * sg
            w = (si * mask).astype(BF)
            fac_ref[t * pairs + c] = (sg + si * (1.0 - sg)) * (mask * DH**-0.5)
            att_ref[t * pairs + c] = w
            attended_ref[r0 : r0 + MAXLEN, lo:hi] = merge(nn(w, v))

    attended = attended_ref[...]
    cen = attended - jnp.mean(attended, axis=1, keepdims=True)
    r = lax.rsqrt(jnp.mean(cen * cen, axis=1, keepdims=True) + EPS)
    yhat = cen * r
    u = act_ref[:, :width].astype(F32)
    gated = (yhat * u).astype(BF)
    gated_ref[...] = gated
    gg = gg_ref[...].astype(F32)
    pg_ref[:, :width] = ((gg * yhat).astype(BF).astype(F32) * dact_ref[:, :width]).astype(BF)
    dy = gg * u
    datt = r * (dy - jnp.mean(dy, axis=1, keepdims=True) - yhat * jnp.mean(dy * yhat, axis=1, keepdims=True))
    attended_ref[...] = datt

    dkv_ref[...] = jnp.zeros_like(dkv_ref)
    for t in range(tiles):
        r0 = t * MAXLEN
        w0 = max(t - 1, 0) * MAXLEN
        for c in range(pairs):
            lo, hi = c * LANES, (c + 1) * LANES
            q = stack(act_ref[r0 : r0 + MAXLEN, 2 * width + lo : 2 * width + hi])
            k = act_ref[w0 : w0 + LANES, 3 * width + lo : 3 * width + hi]
            v = act_ref[w0 : w0 + LANES, width + lo : width + hi]
            da = stack(attended_ref[r0 : r0 + MAXLEN, lo:hi].astype(BF))
            dw = nt(da, v).astype(BF).astype(F32)
            ds = (dw * fac_ref[t * pairs + c]).astype(BF)
            dq = merge(nn(ds, k)).astype(BF).astype(F32)
            qc = slice(2 * width + lo, 2 * width + hi)
            pg_ref[r0 : r0 + MAXLEN, qc] = (dq * dact_ref[r0 : r0 + MAXLEN, qc]).astype(BF)
            dkv_ref[w0 : w0 + LANES, lo:hi] += tn(att_ref[t * pairs + c], da)
            dkv_ref[w0 : w0 + LANES, width + lo : width + hi] += tn(ds, q)
    for g, c in ((1, 0), (3, 1)):
        cols = slice(g * width, (g + 1) * width)
        d = dkv_ref[:, c * width : (c + 1) * width].astype(BF).astype(F32)
        pg_ref[:, cols] = (d * dact_ref[:, cols]).astype(BF)

    dn = nt(pg_ref[...], w_ref[...]).astype(BF).astype(F32)
    dx = rstd * (dn - jnp.mean(dn, axis=1, keepdims=True) - xhat * jnp.mean(dn * xhat, axis=1, keepdims=True))
    in_grad = (dx + outg_ref[...].astype(F32)).astype(BF)

    def position(colour, rel):
        place = 0
        for bit in order[colour]:
            place = place * 2 + ((rel >> bit) & 1)
        return place

    def relative(colour, src):
        tmp_ref[...] = src
        for rel in range(devices):
            at = position(colour, rel) * blk
            src_at = pl.multiple_of((me ^ rel) * blk, blk)
            lhs_ref[at : at + blk, :] = tmp_ref[pl.ds(src_at, blk), :]
        return lhs_ref[...]

    normed_t = jnp.transpose(normed)
    outg_t = jnp.transpose(outg_ref[...])
    if order is None:
        grad_o_ref, grad_u_ref, grad_t_ref = grads
        grad_o_ref[...] = nn(outg_t, gated)
        grad_u_ref[...] = nn(normed_t, pg_ref[...])
        grad_t_ref[...] = nn(jnp.transpose(in_grad), onehot_ref[...]).astype(BF)
        return
    keep1_ref, send1_ref, keep2_ref, send2_ref = grads
    lhs = relative(0, outg_t)
    res = nn(lhs, gated).astype(BF)
    keep1_ref[:, :width] = res[:half]
    send1_ref[:, :width] = res[half:]
    lhs = relative(0, normed_t)
    res = nn(lhs, pg_ref[:, : 2 * width]).astype(BF)
    keep1_ref[:, width:] = res[:half]
    send1_ref[:, width:] = res[half:]
    lhs = relative(1, normed_t)
    res = nn(lhs, pg_ref[:, 2 * width :]).astype(BF)
    keep2_ref[:, : 2 * width] = res[:half]
    send2_ref[:, : 2 * width] = res[half:]
    tmp_ref[...] = jnp.transpose(in_grad)
    feats = width // tabs
    span = items // dps
    for rt in range(tabs):
        at = pl.multiple_of((me_tab ^ rt) * feats, feats)
        lhs_ref[rt * feats : (rt + 1) * feats, :] = tmp_ref[pl.ds(at, feats), :]
    for rd in range(dps):
        at = pl.multiple_of((me_dp ^ rd) * span, span)
        res = nn(lhs_ref[...], onehot_ref[:, pl.ds(at, span)]).astype(BF)
        for rt in range(tabs):
            place = position(1, rd * tabs + rt) * blk
            dst = keep2_ref if place < half else send2_ref
            place = place % half
            for j in range(feats // blk):
                dst[place : place + blk, 2 * width + j * span : 2 * width + (j + 1) * span] = res[
                    rt * feats + j * blk : rt * feats + (j + 1) * blk, :
                ]


def finish_kernel(keep_ref, got_ref, grad_u_ref, grad_o_ref, grad_t_ref):
    blk, width = grad_o_ref.shape
    feats, span = grad_t_ref.shape
    total = keep_ref[...].astype(F32) + got_ref[...].astype(F32)
    grad_o_ref[...] = total[:, :width]
    grad_u_ref[...] = total[:, width : 5 * width]
    for j in range(feats // blk):
        grad_t_ref[j * blk : (j + 1) * blk, :] = total[:, 5 * width + j * span : 5 * width + (j + 1) * span]


VMEM_SPEC = pl.BlockSpec(memory_space=pltpu.VMEM)
HBM_SPEC = pl.BlockSpec(memory_space=pltpu.HBM)


def in_hbm(v):
    return pltpu.with_memory_space_constraint(v, pltpu.HBM)


def swap(v, bit, tab_bits, dps, tabs):
    if bit < tab_bits:
        return lax.ppermute(v, "table", [(i, i ^ (1 << bit)) for i in range(tabs)])
    b = bit - tab_bits
    return lax.ppermute(v, "dp", [(i, i ^ (1 << b)) for i in range(dps)])


def layer(ids, lengths, table, w_uvqk, w_out, cotangent):
    tabs = lax.axis_size("table")
    dps = lax.axis_size("dp")
    devices = tabs * dps
    tab_bits = tabs.bit_length() - 1
    bits = devices.bit_length() - 1
    histories = lengths.shape[1]
    rows = histories * MAXLEN
    live = rows * 5 // 8
    items = table.shape[0]
    feats = table.shape[1]
    width = feats * tabs
    ids2 = ids.reshape(tabs, rows)

    sds = jax.ShapeDtypeStruct

    def other(v, rel):
        return lax.ppermute(v, "table", [(i, i ^ rel) for i in range(tabs)])

    mine = table.T
    far = {}
    for rel in range(2, tabs, 2):
        far[rel] = other(mine, rel)
    onehot, outg, gg, start, origin, w_near, mine_near = pl.pallas_call(
        prep_kernel,
        out_shape=(
            sds((live, items), BF),
            sds((live, width), BF),
            sds((live, width), BF),
            sds((live, LANES), jnp.int32),
            sds((8, live), jnp.int32),
            sds(w_uvqk.shape, BF),
            sds(mine.shape, BF),
        ),
        in_specs=[HBM_SPEC, VMEM_SPEC] + [HBM_SPEC] * 4,
        out_specs=(VMEM_SPEC,) * 7,
        scratch_shapes=[
            pltpu.SMEM(lengths.shape, jnp.int32),
            pltpu.VMEM(cotangent.shape, BF),
            pltpu.VMEM(w_out.shape, BF),
            pltpu.SemaphoreType.DMA((5,)),
        ],
        compiler_params=pltpu.CompilerParams(vmem_limit_bytes=16 << 20),
        name="prep",
    )(in_hbm(lengths), ids2, *map(in_hbm, (cotangent, w_out, w_uvqk, mine)))
    pieces = [mine_near, other(mine, 1)]
    for rel in range(2, tabs, 2):
        pieces += [far[rel], other(far[rel], 1)]

    dp_order = list(range(tab_bits, bits))
    z_order = list(range(1, tab_bits))
    order = ([0] + dp_order + z_order, [0] + dp_order[::-1] + z_order)
    w1 = 3 * width
    blk = width // devices
    span = items // dps
    halving = blk % 16 == 0 and feats % blk == 0 and span == LANES and width % (feats // blk * span) == 0
    if halving:
        grad_shapes = (sds((width // 2, w1), BF),) * 4
    else:
        order = None
        grad_shapes = (sds((width, width), F32), sds((width, 4 * width), F32), sds((width, items), BF))
    tiles = live // MAXLEN * (width // LANES)
    gated, tab_t, *grads = pl.pallas_call(
        functools.partial(layer_kernel, order, (dps, tabs)),
        out_shape=(sds((live, width), BF), sds((width, items), BF)) + grad_shapes,
        in_specs=[VMEM_SPEC] * (5 + tabs),
        out_specs=(VMEM_SPEC,) * (2 + len(grad_shapes)),
        scratch_shapes=[
            pltpu.VMEM((live, 4 * width), BF),
            pltpu.VMEM((live, 4 * width), F32),
            pltpu.VMEM((tiles, LANES, LANES), F32),
            pltpu.VMEM((tiles, LANES, LANES), BF),
            pltpu.VMEM((live, width), F32),
            pltpu.VMEM((live, 2 * width), F32),
            pltpu.VMEM((live, 4 * width), BF),
            pltpu.VMEM((width, live), BF),
            pltpu.VMEM((width, live), BF),
        ],
        compiler_params=pltpu.CompilerParams(vmem_limit_bytes=32 << 20),
        name="layer",
    )(start, onehot, outg, gg, w_near, *pieces)

    def finish_output(gated):
        return pl.pallas_call(
            out_kernel,
            out_shape=sds((rows, width), BF),
            in_specs=[VMEM_SPEC] * 5,
            out_specs=VMEM_SPEC,
            compiler_params=pltpu.CompilerParams(vmem_limit_bytes=16 << 20),
        name="out",
        )(origin, ids2, tab_t, gated, w_out)

    if not halving:
        grad_o, grad_u, grad_t = grads
        grad_t = grad_t.reshape(tabs, feats, dps, span).transpose(2, 0, 1, 3).reshape(devices, feats * span)

        def share(v):
            v = lax.psum_scatter(v, "dp", scatter_dimension=0, tiled=True)
            return lax.psum_scatter(v, "table", scatter_dimension=0, tiled=True)

        return (finish_output(gated), share(grad_t).astype(F32).reshape(feats, span).T, share(grad_u), share(grad_o))

    def add(keep, got):
        return (keep.astype(F32) + got.astype(F32)).astype(BF)

    def halves(v):
        h = v.shape[0] // 2
        return v[:h], v[h:]

    keep1, send1, keep2, send2 = grads
    totals = [add(keep, other(send, 1)) for keep, send in ((keep1, send1), (keep2, send2))]
    gated, *totals = lax.optimization_barrier((gated, *totals))
    output = finish_output(gated)
    for n in range(len(dp_order)):
        for c in range(2):
            keep, send = halves(totals[c])
            totals[c] = add(keep, swap(send, order[c][1 + n], tab_bits, dps, tabs))
        if n == 0:
            output, *totals = lax.optimization_barrier((output, *totals))
    total = jnp.concatenate(totals, axis=1)
    for bit in z_order[:-1]:
        keep, send = halves(total)
        total = add(keep, swap(send, bit, tab_bits, dps, tabs))
    keep, send = halves(total)
    got = swap(send, z_order[-1], tab_bits, dps, tabs)
    grad_uvqk, grad_out_t, grad_t = pl.pallas_call(
        finish_kernel,
        out_shape=(sds((blk, 4 * width), F32), sds((blk, width), F32), sds((feats, span), F32)),
        in_specs=[VMEM_SPEC] * 2,
        out_specs=(VMEM_SPEC,) * 3,
        compiler_params=pltpu.CompilerParams(vmem_limit_bytes=8 << 20),
        name="finish",
    )(keep, got)
    return (output, grad_t.T, grad_uvqk, grad_out_t)


def solution(mesh):
    return jax.shard_map(
        layer,
        mesh=mesh,
        in_specs=(
            P("dp"),
            P(("dp", "table"), None),
            P(None, "table"),
            P(),
            P(),
            P(("dp", "table"), None),
        ),
        out_specs=(
            P(("dp", "table"), None),
            P("dp", "table"),
            P(("dp", "table"), None),
            P(("dp", "table"), None),
        ),
        check_vma=False,
    )
```

```python
import functools
import jax
import jax.numpy as jnp
from jax import lax
from jax.experimental import pallas as pl
from jax.experimental.pallas import tpu as pltpu
from jax.sharding import PartitionSpec as P


DH = 64
MAXLEN = 64
LANES = 128
EPS = 1e-05
SCRATCH = 13
BF = jnp.bfloat16
F32 = jnp.float32


def nt(a, b):
    return lax.dot_general(a, b, (((1,), (1,)), ((), ())), preferred_element_type=F32)


def nn(a, b):
    return jnp.dot(a, b, preferred_element_type=F32)


def sigmoid(v):
    return 0.5 * jnp.tanh(0.5 * v) + 0.5


def origin_of(packed, len_ref, histories):
    shift = jnp.zeros_like(packed)
    end = jnp.int32(0)
    for b in range(histories):
        end = end + len_ref[0, b]
        shift = shift + jnp.where(packed >= end, MAXLEN - len_ref[0, b], 0)
    return packed + shift


def start_of(packed, len_ref, histories):
    start = jnp.zeros_like(packed)
    end = jnp.int32(0)
    for b in range(histories):
        end = end + len_ref[0, b]
        start = jnp.where(packed >= end, end, start)
    return start


def prep_kernel(
    len_hbm, ids_ref, cot_hbm, wout_hbm, w_hbm, mine_hbm,
    onehot_ref, outg_ref, gg_ref, start_ref, origin_ref, w_ref, mine_ref,
    len_ref, cot_ref, wout_ref, sems,
):
    moves = [
        pltpu.make_async_copy(src, dst, sems.at[n])
        for n, (src, dst) in enumerate(
            ((len_hbm, len_ref), (cot_hbm, cot_ref), (wout_hbm, wout_ref), (w_hbm, w_ref), (mine_hbm, mine_ref))
        )
    ]
    for move in moves:
        move.start()
    histories = len_ref.shape[1]
    live, items = onehot_ref.shape
    rows = ids_ref.shape[1]
    own = lax.axis_index("table")
    ids = ids_ref[pl.ds(own, 1), :].astype(F32)
    moves[0].wait()
    start_ref[...] = start_of(lax.broadcasted_iota(jnp.int32, start_ref.shape, 0), len_ref, histories)
    origin_ref[...] = origin_of(lax.broadcasted_iota(jnp.int32, origin_ref.shape, 1), len_ref, histories)
    packed = lax.broadcasted_iota(jnp.int32, (live, rows), 0)
    take = origin_of(packed, len_ref, histories) == lax.broadcasted_iota(jnp.int32, (live, rows), 1)
    own_id = jnp.sum(jnp.where(take, ids, 0.0), axis=1, keepdims=True).astype(jnp.int32)
    onehot_ref[...] = jnp.where(
        lax.broadcasted_iota(jnp.int32, (live, items), 1) == own_id, 1.0, 0.0
    ).astype(BF)
    moves[1].wait()
    out_grad = nn(jnp.where(take, 1.0, 0.0).astype(BF), cot_ref[...]).astype(BF)
    outg_ref[...] = out_grad
    moves[2].wait()
    gg_ref[...] = nt(out_grad, wout_ref[...]).astype(BF)
    moves[3].wait()
    moves[4].wait()


def out_kernel(origin_ref, ids_ref, tab_ref, gated_ref, wout_ref, out_ref):
    rows = ids_ref.shape[1]
    live = gated_ref.shape[0]
    items = tab_ref.shape[1]
    own = lax.axis_index("table")
    ids = ids_ref[pl.ds(own, 1), :].astype(F32)
    ids_col = jnp.transpose(jnp.broadcast_to(ids, (LANES, rows))).astype(jnp.int32)
    lane = lax.broadcasted_iota(jnp.int32, (rows, LANES), 1)
    onehot = jnp.concatenate(
        [jnp.where(ids_col == lane + k, 1.0, 0.0).astype(BF) for k in range(0, items, LANES)], axis=1
    )
    put = origin_ref[0:1, :] == lax.broadcasted_iota(jnp.int32, (rows, live), 0)
    gated = nn(jnp.where(put, 1.0, 0.0).astype(BF), gated_ref[...]).astype(BF)
    out_ref[...] = (nt(onehot, tab_ref[...]) + nn(gated, wout_ref[...])).astype(BF)


def layer_kernel(order, shape, start_ref, onehot_ref, outg_ref, gg_ref, w_ref, *refs):
    _, tabs = shape
    pieces, refs = refs[:tabs], refs[tabs:]
    gated_ref, tab_ref = refs[:2]
    grads, scratch = refs[2:-SCRATCH], refs[-SCRATCH:]
    me_tab = lax.axis_index("table")
    for rel in range(tabs):
        feats = pieces[rel].shape[0]
        at = pl.multiple_of((me_tab ^ rel) * feats, feats)
        tab_ref[pl.ds(at, feats), :] = pieces[rel][...]
    layer_body(order, shape, start_ref, tab_ref, onehot_ref, outg_ref, gg_ref, w_ref, gated_ref, grads, *scratch)


def layer_body(
    order, shape, start_ref, tab_ref, onehot_ref, outg_ref, gg_ref, w_ref, gated_ref, grads,
    act_ref, dact_ref, sc_ref, fac_ref, qs_ref, das_ref, att_ref, ds_ref, turned_ref,
    attended_ref, pg_ref, tmp_ref, lhs_ref,
):
    live, items = onehot_ref.shape
    width = tab_ref.shape[0]
    dps, tabs = shape
    devices = dps * tabs
    me_dp = lax.axis_index("dp")
    me_tab = lax.axis_index("table")
    me = me_dp * tabs + me_tab
    blk = width // devices
    half = width // 2

    x = nt(onehot_ref[...], tab_ref[...])
    centred = x - jnp.mean(x, axis=1, keepdims=True)
    rstd = lax.rsqrt(jnp.mean(centred * centred, axis=1, keepdims=True) + EPS)
    xhat = centred * rstd
    normed = xhat.astype(BF)
    for g in range(4):
        cols = slice(g * width, (g + 1) * width)
        p = nn(normed, w_ref[:, cols])
        s = sigmoid(p)
        a = p * s
        act_ref[:, cols] = a.astype(BF)
        dact_ref[:, cols] = s + a * (1.0 - s)

    tiles = live // MAXLEN
    pairs = width // LANES
    low = lax.broadcasted_iota(jnp.int32, (MAXLEN, LANES), 1) < DH
    zero = jnp.zeros((MAXLEN, LANES), BF)

    def stack(v):
        return jnp.concatenate([jnp.where(low, v, zero), jnp.where(low, zero, v)], axis=0)

    def merge(v):
        return jnp.where(low, v[:MAXLEN], v[MAXLEN:])

    spots = [
        (t * pairs + c, t * MAXLEN, max(t - 1, 0) * MAXLEN, c * LANES) for t in range(tiles) for c in range(pairs)
    ]
    for n, r0, w0, lo in spots:
        q = stack(act_ref[r0 : r0 + MAXLEN, 2 * width + lo : 2 * width + lo + LANES])
        qs_ref[n] = q
        sc_ref[n] = nt(q, act_ref[w0 : w0 + LANES, 3 * width + lo : 3 * width + lo + LANES])
    for t in range(tiles):
        r0 = t * MAXLEN
        row = r0 + lax.broadcasted_iota(jnp.int32, (MAXLEN, LANES), 0)
        col = max(t - 1, 0) * MAXLEN + lax.broadcasted_iota(jnp.int32, (MAXLEN, LANES), 1)
        seen = (col >= start_ref[r0 : r0 + MAXLEN, :]) & (col <= row)
        mask = jnp.where(seen, 1.0 / MAXLEN, 0.0)
        mask = jnp.concatenate([mask, mask], axis=0)
        slope = mask * DH**-0.5
        for c in range(pairs):
            n = t * pairs + c
            sc = sc_ref[n] * DH**-0.5
            sg = sigmoid(sc)
            si = sc * sg
            att_ref[n * LANES : (n + 1) * LANES, :] = (si * mask).astype(BF)
            fac_ref[n] = (sg + si * (1.0 - sg)) * slope
    for n, r0, w0, lo in spots:
        v = act_ref[w0 : w0 + LANES, width + lo : width + lo + LANES]
        attended_ref[r0 : r0 + MAXLEN, lo : lo + LANES] = merge(nn(att_ref[n * LANES : (n + 1) * LANES, :], v))

    attended = attended_ref[...]
    cen = attended - jnp.mean(attended, axis=1, keepdims=True)
    r = lax.rsqrt(jnp.mean(cen * cen, axis=1, keepdims=True) + EPS)
    yhat = cen * r
    u = act_ref[:, :width].astype(F32)
    gated = (yhat * u).astype(BF)
    gated_ref[...] = gated
    gg = gg_ref[...].astype(F32)
    pg_ref[:, :width] = ((gg * yhat).astype(BF).astype(F32) * dact_ref[:, :width]).astype(BF)
    dy = gg * u
    datt = r * (dy - jnp.mean(dy, axis=1, keepdims=True) - yhat * jnp.mean(dy * yhat, axis=1, keepdims=True))
    attended_ref[...] = datt

    for n, r0, w0, lo in spots:
        da = stack(attended_ref[r0 : r0 + MAXLEN, lo : lo + LANES].astype(BF))
        das_ref[n] = da
        sc_ref[n] = nt(da, act_ref[w0 : w0 + LANES, width + lo : width + lo + LANES])
    for n in range(tiles * pairs):
        dw = sc_ref[n].astype(BF).astype(F32)
        ds_ref[n * LANES : (n + 1) * LANES, :] = (dw * fac_ref[n]).astype(BF)
    for n, r0, w0, lo in spots:
        k = act_ref[w0 : w0 + LANES, 3 * width + lo : 3 * width + lo + LANES]
        dq = merge(nn(ds_ref[n * LANES : (n + 1) * LANES, :], k)).astype(BF).astype(F32)
        qc = slice(2 * width + lo, 2 * width + lo + LANES)
        pg_ref[r0 : r0 + MAXLEN, qc] = (dq * dact_ref[r0 : r0 + MAXLEN, qc]).astype(BF)
    for src_ref, rhs_ref, g in ((att_ref, das_ref, 1), (ds_ref, qs_ref, 3)):
        turned_ref[...] = jnp.transpose(src_ref[...])
        for t in range(tiles):
            off = MAXLEN if t else 0
            for c in range(pairs):
                n = t * pairs + c
                lhs = turned_ref[off : off + MAXLEN, n * LANES : (n + 1) * LANES]
                rhs = rhs_ref[n]
                if t + 1 < tiles:
                    m = n + pairs
                    lhs = jnp.concatenate([lhs, turned_ref[:MAXLEN, m * LANES : (m + 1) * LANES]], axis=1)
                    rhs = jnp.concatenate([rhs, rhs_ref[m]], axis=0)
                cols = slice(g * width + c * LANES, g * width + (c + 1) * LANES)
                rows = slice(t * MAXLEN, (t + 1) * MAXLEN)
                d = nn(lhs, rhs).astype(BF).astype(F32)
                pg_ref[rows, cols] = (d * dact_ref[rows, cols]).astype(BF)

    dn = nt(pg_ref[...], w_ref[...]).astype(BF).astype(F32)
    dx = rstd * (dn - jnp.mean(dn, axis=1, keepdims=True) - xhat * jnp.mean(dn * xhat, axis=1, keepdims=True))
    in_grad = (dx + outg_ref[...].astype(F32)).astype(BF)

    def position(colour, rel):
        place = 0
        for bit in order[colour]:
            place = place * 2 + ((rel >> bit) & 1)
        return place

    def relative(colour, src):
        tmp_ref[...] = src
        for rel in range(devices):
            at = position(colour, rel) * blk
            src_at = pl.multiple_of((me ^ rel) * blk, blk)
            lhs_ref[at : at + blk, :] = tmp_ref[pl.ds(src_at, blk), :]
        return lhs_ref[...]

    normed_t = jnp.transpose(normed)
    outg_t = jnp.transpose(outg_ref[...])
    if order is None:
        grad_o_ref, grad_u_ref, grad_t_ref = grads
        grad_o_ref[...] = nn(outg_t, gated)
        grad_u_ref[...] = nn(normed_t, pg_ref[...])
        grad_t_ref[...] = nn(jnp.transpose(in_grad), onehot_ref[...]).astype(BF)
        return

    def emit(colour, at, lhs, rhs):
        res = nn(lhs, rhs).astype(BF)
        cols = slice(at, at + rhs.shape[1])
        grads[2 * colour][:, cols] = res[:half]
        grads[2 * colour + 1][:, cols] = res[half:]

    emit(0, 0, relative(0, outg_t), gated)
    emit(0, width, relative(0, normed_t), pg_ref[:, :width])
    emit(1, 0, relative(1, normed_t), pg_ref[:, width : 3 * width])
    emit(2, 0, relative(2, normed_t), pg_ref[:, 3 * width :])
    tmp_ref[...] = jnp.transpose(in_grad)
    feats = width // tabs
    span = items // dps
    for rt in range(tabs):
        at = pl.multiple_of((me_tab ^ rt) * feats, feats)
        lhs_ref[rt * feats : (rt + 1) * feats, :] = tmp_ref[pl.ds(at, feats), :]
    for rd in range(dps):
        at = pl.multiple_of((me_dp ^ rd) * span, span)
        res = nn(lhs_ref[...], onehot_ref[:, pl.ds(at, span)]).astype(BF)
        for rt in range(tabs):
            place = position(2, rd * tabs + rt) * blk
            dst = grads[4] if place < half else grads[5]
            place = place % half
            for j in range(feats // blk):
                dst[place : place + blk, width + j * span : width + (j + 1) * span] = res[
                    rt * feats + j * blk : rt * feats + (j + 1) * blk, :
                ]


def finish_kernel(keep_ref, got_ref, grad_u_ref, grad_o_ref, grad_t_ref):
    blk, width = grad_o_ref.shape
    feats, span = grad_t_ref.shape
    total = keep_ref[...].astype(F32) + got_ref[...].astype(F32)
    grad_o_ref[...] = total[:, :width]
    grad_u_ref[...] = total[:, width : 5 * width]
    for j in range(feats // blk):
        grad_t_ref[j * blk : (j + 1) * blk, :] = total[:, 5 * width + j * span : 5 * width + (j + 1) * span]


VMEM_SPEC = pl.BlockSpec(memory_space=pltpu.VMEM)
HBM_SPEC = pl.BlockSpec(memory_space=pltpu.HBM)


def in_hbm(v):
    return pltpu.with_memory_space_constraint(v, pltpu.HBM)


def swap(v, bit, tab_bits, dps, tabs):
    if bit < tab_bits:
        return lax.ppermute(v, "table", [(i, i ^ (1 << bit)) for i in range(tabs)])
    b = bit - tab_bits
    return lax.ppermute(v, "dp", [(i, i ^ (1 << b)) for i in range(dps)])


def layer(ids, lengths, table, w_uvqk, w_out, cotangent):
    tabs = lax.axis_size("table")
    dps = lax.axis_size("dp")
    devices = tabs * dps
    tab_bits = tabs.bit_length() - 1
    bits = devices.bit_length() - 1
    histories = lengths.shape[1]
    rows = histories * MAXLEN
    live = rows * 5 // 8
    items = table.shape[0]
    feats = table.shape[1]
    width = feats * tabs
    ids2 = ids.reshape(tabs, rows)

    sds = jax.ShapeDtypeStruct

    def other(v, rel):
        return lax.ppermute(v, "table", [(i, i ^ rel) for i in range(tabs)])

    mine = table.T
    far = {}
    for rel in range(2, tabs, 2):
        far[rel] = other(mine, rel)
    onehot, outg, gg, start, origin, w_near, mine_near = pl.pallas_call(
        prep_kernel,
        out_shape=(
            sds((live, items), BF),
            sds((live, width), BF),
            sds((live, width), BF),
            sds((live, LANES), jnp.int32),
            sds((8, live), jnp.int32),
            sds(w_uvqk.shape, BF),
            sds(mine.shape, BF),
        ),
        in_specs=[HBM_SPEC, VMEM_SPEC] + [HBM_SPEC] * 4,
        out_specs=(VMEM_SPEC,) * 7,
        scratch_shapes=[
            pltpu.SMEM(lengths.shape, jnp.int32),
            pltpu.VMEM(cotangent.shape, BF),
            pltpu.VMEM(w_out.shape, BF),
            pltpu.SemaphoreType.DMA((5,)),
        ],
        compiler_params=pltpu.CompilerParams(vmem_limit_bytes=16 << 20),
        name="prep",
    )(in_hbm(lengths), ids2, *map(in_hbm, (cotangent, w_out, w_uvqk, mine)))
    pieces = [mine_near, other(mine, 1)]
    for rel in range(2, tabs, 2):
        pieces += [far[rel], other(far[rel], 1)]

    ring = list(range(tab_bits, bits)) + list(range(1, tab_bits - 1))
    colours = 3
    order = [[0] + ring[c:] + ring[:c] + [tab_bits - 1] for c in range(colours)]
    w1 = 2 * width
    blk = width // devices
    span = items // dps
    halving = blk % 16 == 0 and feats % blk == 0 and span == LANES and width % (feats // blk * span) == 0
    if halving:
        grad_shapes = (sds((width // 2, w1), BF),) * (2 * colours)
    else:
        order = None
        grad_shapes = (sds((width, width), F32), sds((width, 4 * width), F32), sds((width, items), BF))
    tiles = live // MAXLEN * (width // LANES)
    gated, tab_t, *grads = pl.pallas_call(
        functools.partial(layer_kernel, order, (dps, tabs)),
        out_shape=(sds((live, width), BF), sds((width, items), BF)) + grad_shapes,
        in_specs=[VMEM_SPEC] * (5 + tabs),
        out_specs=(VMEM_SPEC,) * (2 + len(grad_shapes)),
        scratch_shapes=[
            pltpu.VMEM((live, 4 * width), BF),
            pltpu.VMEM((live, 4 * width), F32),
            pltpu.VMEM((tiles, LANES, LANES), F32),
            pltpu.VMEM((tiles, LANES, LANES), F32),
            pltpu.VMEM((tiles, LANES, LANES), BF),
            pltpu.VMEM((tiles, LANES, LANES), BF),
            pltpu.VMEM((tiles * LANES, LANES), BF),
            pltpu.VMEM((tiles * LANES, LANES), BF),
            pltpu.VMEM((LANES, tiles * LANES), BF),
            pltpu.VMEM((live, width), F32),
            pltpu.VMEM((live, 4 * width), BF),
            pltpu.VMEM((width, live), BF),
            pltpu.VMEM((width, live), BF),
        ],
        compiler_params=pltpu.CompilerParams(vmem_limit_bytes=32 << 20),
        name="layer",
    )(start, onehot, outg, gg, w_near, *pieces)

    def finish_output(gated):
        return pl.pallas_call(
            out_kernel,
            out_shape=sds((rows, width), BF),
            in_specs=[VMEM_SPEC] * 5,
            out_specs=VMEM_SPEC,
            compiler_params=pltpu.CompilerParams(vmem_limit_bytes=16 << 20),
        name="out",
        )(origin, ids2, tab_t, gated, w_out)

    if not halving:
        grad_o, grad_u, grad_t = grads
        grad_t = grad_t.reshape(tabs, feats, dps, span).transpose(2, 0, 1, 3).reshape(devices, feats * span)

        def share(v):
            v = lax.psum_scatter(v, "dp", scatter_dimension=0, tiled=True)
            return lax.psum_scatter(v, "table", scatter_dimension=0, tiled=True)

        return (finish_output(gated), share(grad_t).astype(F32).reshape(feats, span).T, share(grad_u), share(grad_o))

    def add(keep, got):
        return (keep.astype(F32) + got.astype(F32)).astype(BF)

    def halves(v):
        h = v.shape[0] // 2
        return v[:h], v[h:]

    totals = [add(keep, other(send, 1)) for keep, send in zip(grads[::2], grads[1::2])]
    gated, *totals = lax.optimization_barrier((gated, *totals))
    output = finish_output(gated)
    for n in range(len(ring)):
        for c in range(colours):
            keep, send = halves(totals[c])
            totals[c] = add(keep, swap(send, order[c][1 + n], tab_bits, dps, tabs))
        if n == 0:
            output, *totals = lax.optimization_barrier((output, *totals))
    keep, send = halves(jnp.concatenate(totals, axis=1))
    got = swap(send, tab_bits - 1, tab_bits, dps, tabs)
    grad_uvqk, grad_out_t, grad_t = pl.pallas_call(
        finish_kernel,
        out_shape=(sds((blk, 4 * width), F32), sds((blk, width), F32), sds((feats, span), F32)),
        in_specs=[VMEM_SPEC] * 2,
        out_specs=(VMEM_SPEC,) * 3,
        compiler_params=pltpu.CompilerParams(vmem_limit_bytes=8 << 20),
        name="finish",
    )(keep, got)
    return (output, grad_t.T, grad_uvqk, grad_out_t)


def solution(mesh):
    return jax.shard_map(
        layer,
        mesh=mesh,
        in_specs=(
            P("dp"),
            P(("dp", "table"), None),
            P(None, "table"),
            P(),
            P(),
            P(("dp", "table"), None),
        ),
        out_specs=(
            P(("dp", "table"), None),
            P("dp", "table"),
            P(("dp", "table"), None),
            P(("dp", "table"), None),
        ),
        check_vma=False,
    )
```

```python
import functools
import jax
import jax.numpy as jnp
from jax import lax
from jax.experimental import pallas as pl
from jax.experimental.pallas import tpu as pltpu
from jax.sharding import PartitionSpec as P


DH = 64
MAXLEN = 64
LANES = 128
EPS = 1e-05
SCRATCH = 13
BF = jnp.bfloat16
F32 = jnp.float32


def nt(a, b):
    return lax.dot_general(a, b, (((1,), (1,)), ((), ())), preferred_element_type=F32)


def nn(a, b):
    return jnp.dot(a, b, preferred_element_type=F32)


def sigmoid(v):
    return 0.5 * jnp.tanh(0.5 * v) + 0.5


def origin_of(packed, len_ref, histories):
    shift = jnp.zeros_like(packed)
    end = jnp.int32(0)
    for b in range(histories):
        end = end + len_ref[0, b]
        shift = shift + jnp.where(packed >= end, MAXLEN - len_ref[0, b], 0)
    return packed + shift


def start_of(packed, len_ref, histories):
    start = jnp.zeros_like(packed)
    end = jnp.int32(0)
    for b in range(histories):
        end = end + len_ref[0, b]
        start = jnp.where(packed >= end, end, start)
    return start


def prep_kernel(
    len_hbm, ids_ref, cot_hbm, wout_hbm, w_hbm, mine_hbm,
    onehot_ref, outg_ref, gg_ref, start_ref, origin_ref, w_ref, mine_ref,
    len_ref, cot_ref, wout_ref, sems,
):
    moves = [
        pltpu.make_async_copy(src, dst, sems.at[n])
        for n, (src, dst) in enumerate(
            ((len_hbm, len_ref), (cot_hbm, cot_ref), (wout_hbm, wout_ref), (w_hbm, w_ref), (mine_hbm, mine_ref))
        )
    ]
    for move in moves:
        move.start()
    histories = len_ref.shape[1]
    live, items = onehot_ref.shape
    rows = ids_ref.shape[1]
    own = lax.axis_index("table")
    ids = ids_ref[pl.ds(own, 1), :].astype(F32)
    moves[0].wait()
    start_ref[...] = start_of(lax.broadcasted_iota(jnp.int32, start_ref.shape, 0), len_ref, histories)
    origin_ref[...] = origin_of(lax.broadcasted_iota(jnp.int32, origin_ref.shape, 1), len_ref, histories)
    packed = lax.broadcasted_iota(jnp.int32, (live, rows), 0)
    take = origin_of(packed, len_ref, histories) == lax.broadcasted_iota(jnp.int32, (live, rows), 1)
    own_id = jnp.sum(jnp.where(take, ids, 0.0), axis=1, keepdims=True).astype(jnp.int32)
    onehot_ref[...] = jnp.where(
        lax.broadcasted_iota(jnp.int32, (live, items), 1) == own_id, 1.0, 0.0
    ).astype(BF)
    moves[1].wait()
    out_grad = nn(jnp.where(take, 1.0, 0.0).astype(BF), cot_ref[...]).astype(BF)
    outg_ref[...] = out_grad
    moves[2].wait()
    gg_ref[...] = nt(out_grad, wout_ref[...]).astype(BF)
    moves[3].wait()
    moves[4].wait()


def out_kernel(origin_ref, ids_ref, tab_ref, gated_ref, wout_ref, out_ref):
    rows = ids_ref.shape[1]
    live = gated_ref.shape[0]
    items = tab_ref.shape[1]
    own = lax.axis_index("table")
    ids = ids_ref[pl.ds(own, 1), :].astype(F32)
    ids_col = jnp.transpose(jnp.broadcast_to(ids, (LANES, rows))).astype(jnp.int32)
    lane = lax.broadcasted_iota(jnp.int32, (rows, LANES), 1)
    onehot = jnp.concatenate(
        [jnp.where(ids_col == lane + k, 1.0, 0.0).astype(BF) for k in range(0, items, LANES)], axis=1
    )
    put = origin_ref[0:1, :] == lax.broadcasted_iota(jnp.int32, (rows, live), 0)
    gated = nn(jnp.where(put, 1.0, 0.0).astype(BF), gated_ref[...]).astype(BF)
    out_ref[...] = (nt(onehot, tab_ref[...]) + nn(gated, wout_ref[...])).astype(BF)


def layer_kernel(order, shape, start_ref, onehot_ref, outg_ref, gg_ref, w_ref, *refs):
    _, tabs = shape
    pieces, refs = refs[:tabs], refs[tabs:]
    gated_ref, tab_ref = refs[:2]
    grads, scratch = refs[2:-SCRATCH], refs[-SCRATCH:]
    me_tab = lax.axis_index("table")
    for rel in range(tabs):
        feats = pieces[rel].shape[0]
        at = pl.multiple_of((me_tab ^ rel) * feats, feats)
        tab_ref[pl.ds(at, feats), :] = pieces[rel][...]
    layer_body(order, shape, start_ref, tab_ref, onehot_ref, outg_ref, gg_ref, w_ref, gated_ref, grads, *scratch)


def layer_body(
    order, shape, start_ref, tab_ref, onehot_ref, outg_ref, gg_ref, w_ref, gated_ref, grads,
    act_ref, dact_ref, sc_ref, fac_ref, qs_ref, das_ref, att_ref, ds_ref, turned_ref,
    attended_ref, pg_ref, tmp_ref, lhs_ref,
):
    live, items = onehot_ref.shape
    width = tab_ref.shape[0]
    dps, tabs = shape
    devices = dps * tabs
    me_dp = lax.axis_index("dp")
    me_tab = lax.axis_index("table")
    me = me_dp * tabs + me_tab
    blk = width // devices
    half = width // 2

    x = nt(onehot_ref[...], tab_ref[...])
    centred = x - jnp.mean(x, axis=1, keepdims=True)
    rstd = lax.rsqrt(jnp.mean(centred * centred, axis=1, keepdims=True) + EPS)
    xhat = centred * rstd
    normed = xhat.astype(BF)
    for g in range(4):
        cols = slice(g * width, (g + 1) * width)
        p = nn(normed, w_ref[:, cols])
        s = sigmoid(p)
        a = p * s
        act_ref[:, cols] = a.astype(BF)
        dact_ref[:, cols] = s + a * (1.0 - s)

    tiles = live // MAXLEN
    pairs = width // LANES
    low = lax.broadcasted_iota(jnp.int32, (MAXLEN, LANES), 1) < DH
    zero = jnp.zeros((MAXLEN, LANES), BF)

    def stack(v):
        return jnp.concatenate([jnp.where(low, v, zero), jnp.where(low, zero, v)], axis=0)

    def merge(v):
        return jnp.where(low, v[:MAXLEN], v[MAXLEN:])

    spots = [
        (t * pairs + c, t * MAXLEN, max(t - 1, 0) * MAXLEN, c * LANES) for t in range(tiles) for c in range(pairs)
    ]
    for n, r0, w0, lo in spots:
        q = stack(act_ref[r0 : r0 + MAXLEN, 2 * width + lo : 2 * width + lo + LANES])
        qs_ref[n] = q
        sc_ref[n] = nt(q, act_ref[w0 : w0 + LANES, 3 * width + lo : 3 * width + lo + LANES])
    for t in range(tiles):
        r0 = t * MAXLEN
        row = r0 + lax.broadcasted_iota(jnp.int32, (MAXLEN, LANES), 0)
        col = max(t - 1, 0) * MAXLEN + lax.broadcasted_iota(jnp.int32, (MAXLEN, LANES), 1)
        seen = (col >= start_ref[r0 : r0 + MAXLEN, :]) & (col <= row)
        mask = jnp.where(seen, 1.0 / MAXLEN, 0.0)
        mask = jnp.concatenate([mask, mask], axis=0)
        slope = mask * DH**-0.5
        for c in range(pairs):
            n = t * pairs + c
            sc = sc_ref[n] * DH**-0.5
            sg = sigmoid(sc)
            si = sc * sg
            att_ref[n * LANES : (n + 1) * LANES, :] = (si * mask).astype(BF)
            fac_ref[n] = (sg + si * (1.0 - sg)) * slope
    for n, r0, w0, lo in spots:
        v = act_ref[w0 : w0 + LANES, width + lo : width + lo + LANES]
        attended_ref[r0 : r0 + MAXLEN, lo : lo + LANES] = merge(nn(att_ref[n * LANES : (n + 1) * LANES, :], v))

    attended = attended_ref[...]
    cen = attended - jnp.mean(attended, axis=1, keepdims=True)
    r = lax.rsqrt(jnp.mean(cen * cen, axis=1, keepdims=True) + EPS)
    yhat = cen * r
    u = act_ref[:, :width].astype(F32)
    gated = (yhat * u).astype(BF)
    gated_ref[...] = gated
    gg = gg_ref[...].astype(F32)
    pg_ref[:, :width] = ((gg * yhat).astype(BF).astype(F32) * dact_ref[:, :width]).astype(BF)
    dy = gg * u
    datt = r * (dy - jnp.mean(dy, axis=1, keepdims=True) - yhat * jnp.mean(dy * yhat, axis=1, keepdims=True))
    attended_ref[...] = datt

    for n, r0, w0, lo in spots:
        da = stack(attended_ref[r0 : r0 + MAXLEN, lo : lo + LANES].astype(BF))
        das_ref[n] = da
        sc_ref[n] = nt(da, act_ref[w0 : w0 + LANES, width + lo : width + lo + LANES])
    for n in range(tiles * pairs):
        dw = sc_ref[n].astype(BF).astype(F32)
        ds_ref[n * LANES : (n + 1) * LANES, :] = (dw * fac_ref[n]).astype(BF)
    for n, r0, w0, lo in spots:
        k = act_ref[w0 : w0 + LANES, 3 * width + lo : 3 * width + lo + LANES]
        dq = merge(nn(ds_ref[n * LANES : (n + 1) * LANES, :], k)).astype(BF).astype(F32)
        qc = slice(2 * width + lo, 2 * width + lo + LANES)
        pg_ref[r0 : r0 + MAXLEN, qc] = (dq * dact_ref[r0 : r0 + MAXLEN, qc]).astype(BF)
    for src_ref, rhs_ref, g in ((att_ref, das_ref, 1), (ds_ref, qs_ref, 3)):
        turned_ref[...] = jnp.transpose(src_ref[...])
        for t in range(tiles):
            off = MAXLEN if t else 0
            for c in range(pairs):
                n = t * pairs + c
                lhs = turned_ref[off : off + MAXLEN, n * LANES : (n + 1) * LANES]
                rhs = rhs_ref[n]
                if t + 1 < tiles:
                    m = n + pairs
                    lhs = jnp.concatenate([lhs, turned_ref[:MAXLEN, m * LANES : (m + 1) * LANES]], axis=1)
                    rhs = jnp.concatenate([rhs, rhs_ref[m]], axis=0)
                cols = slice(g * width + c * LANES, g * width + (c + 1) * LANES)
                rows = slice(t * MAXLEN, (t + 1) * MAXLEN)
                d = nn(lhs, rhs).astype(BF).astype(F32)
                pg_ref[rows, cols] = (d * dact_ref[rows, cols]).astype(BF)

    dn = nt(pg_ref[...], w_ref[...]).astype(BF).astype(F32)
    dx = rstd * (dn - jnp.mean(dn, axis=1, keepdims=True) - xhat * jnp.mean(dn * xhat, axis=1, keepdims=True))
    in_grad = (dx + outg_ref[...].astype(F32)).astype(BF)

    def position(colour, rel):
        place = 0
        for bit in order[colour]:
            place = place * 2 + ((rel >> bit) & 1)
        return place

    def relative(colour, src):
        tmp_ref[...] = src
        for rel in range(devices):
            at = position(colour, rel) * blk
            src_at = pl.multiple_of((me ^ rel) * blk, blk)
            lhs_ref[at : at + blk, :] = tmp_ref[pl.ds(src_at, blk), :]
        return lhs_ref[...]

    normed_t = jnp.transpose(normed)
    outg_t = jnp.transpose(outg_ref[...])
    if order is None:
        grad_o_ref, grad_u_ref, grad_t_ref = grads
        grad_o_ref[...] = nn(outg_t, gated)
        grad_u_ref[...] = nn(normed_t, pg_ref[...])
        grad_t_ref[...] = nn(jnp.transpose(in_grad), onehot_ref[...]).astype(BF)
        return

    def emit(colour, at, lhs, rhs):
        res = nn(lhs, rhs).astype(BF)
        cols = slice(at, at + rhs.shape[1])
        grads[2 * colour][:, cols] = res[:half]
        grads[2 * colour + 1][:, cols] = res[half:]

    emit(0, 0, relative(0, outg_t), gated)
    emit(0, width, relative(0, normed_t), pg_ref[:, :width])
    emit(1, 0, relative(1, normed_t), pg_ref[:, width : 3 * width])
    emit(2, 0, relative(2, normed_t), pg_ref[:, 3 * width :])
    tmp_ref[...] = jnp.transpose(in_grad)
    feats = width // tabs
    span = items // dps
    for rt in range(tabs):
        at = pl.multiple_of((me_tab ^ rt) * feats, feats)
        lhs_ref[rt * feats : (rt + 1) * feats, :] = tmp_ref[pl.ds(at, feats), :]
    for rd in range(dps):
        at = pl.multiple_of((me_dp ^ rd) * span, span)
        res = nn(lhs_ref[...], onehot_ref[:, pl.ds(at, span)]).astype(BF)
        for rt in range(tabs):
            place = position(2, rd * tabs + rt) * blk
            dst = grads[4] if place < half else grads[5]
            place = place % half
            for j in range(feats // blk):
                dst[place : place + blk, width + j * span : width + (j + 1) * span] = res[
                    rt * feats + j * blk : rt * feats + (j + 1) * blk, :
                ]


def finish_kernel(*refs):
    grad_u_ref, grad_o_ref, grad_t_ref = refs[-3:]
    blk, width = grad_o_ref.shape
    feats, span = grad_t_ref.shape
    first, second, third = (refs[n][...].astype(F32) + refs[n + 1][...].astype(F32) for n in range(0, 6, 2))
    grad_o_ref[...] = first[:, :width]
    grad_u_ref[:, :width] = first[:, width:]
    grad_u_ref[:, width : 3 * width] = second
    grad_u_ref[:, 3 * width :] = third[:, :width]
    for j in range(feats // blk):
        grad_t_ref[j * blk : (j + 1) * blk, :] = third[:, width + j * span : width + (j + 1) * span]


VMEM_SPEC = pl.BlockSpec(memory_space=pltpu.VMEM)
HBM_SPEC = pl.BlockSpec(memory_space=pltpu.HBM)


def in_hbm(v):
    return pltpu.with_memory_space_constraint(v, pltpu.HBM)


def swap(v, bit, tab_bits, dps, tabs):
    if bit < tab_bits:
        return lax.ppermute(v, "table", [(i, i ^ (1 << bit)) for i in range(tabs)])
    b = bit - tab_bits
    return lax.ppermute(v, "dp", [(i, i ^ (1 << b)) for i in range(dps)])


def layer(ids, lengths, table, w_uvqk, w_out, cotangent):
    tabs = lax.axis_size("table")
    dps = lax.axis_size("dp")
    devices = tabs * dps
    tab_bits = tabs.bit_length() - 1
    bits = devices.bit_length() - 1
    histories = lengths.shape[1]
    rows = histories * MAXLEN
    live = rows * 5 // 8
    items = table.shape[0]
    feats = table.shape[1]
    width = feats * tabs
    ids2 = ids.reshape(tabs, rows)

    sds = jax.ShapeDtypeStruct

    def other(v, rel):
        return lax.ppermute(v, "table", [(i, i ^ rel) for i in range(tabs)])

    mine = table.T
    far = {}
    for rel in range(2, tabs, 2):
        far[rel] = other(mine, rel)
    onehot, outg, gg, start, origin, w_near, mine_near = pl.pallas_call(
        prep_kernel,
        out_shape=(
            sds((live, items), BF),
            sds((live, width), BF),
            sds((live, width), BF),
            sds((live, LANES), jnp.int32),
            sds((8, live), jnp.int32),
            sds(w_uvqk.shape, BF),
            sds(mine.shape, BF),
        ),
        in_specs=[HBM_SPEC, VMEM_SPEC] + [HBM_SPEC] * 4,
        out_specs=(VMEM_SPEC,) * 7,
        scratch_shapes=[
            pltpu.SMEM(lengths.shape, jnp.int32),
            pltpu.VMEM(cotangent.shape, BF),
            pltpu.VMEM(w_out.shape, BF),
            pltpu.SemaphoreType.DMA((5,)),
        ],
        compiler_params=pltpu.CompilerParams(vmem_limit_bytes=16 << 20),
        name="prep",
    )(in_hbm(lengths), ids2, *map(in_hbm, (cotangent, w_out, w_uvqk, mine)))
    pieces = [mine_near, other(mine, 1)]
    for rel in range(2, tabs, 2):
        pieces += [far[rel], other(far[rel], 1)]

    ring = list(range(tab_bits, bits)) + list(range(1, tab_bits - 1))
    colours = 3
    order = [[0] + ring[c:] + ring[:c] + [tab_bits - 1] for c in range(colours)]
    w1 = 2 * width
    blk = width // devices
    span = items // dps
    halving = blk % 16 == 0 and feats % blk == 0 and span == LANES and width % (feats // blk * span) == 0
    if halving:
        grad_shapes = (sds((width // 2, w1), BF),) * (2 * colours)
    else:
        order = None
        grad_shapes = (sds((width, width), F32), sds((width, 4 * width), F32), sds((width, items), BF))
    tiles = live // MAXLEN * (width // LANES)
    gated, tab_t, *grads = pl.pallas_call(
        functools.partial(layer_kernel, order, (dps, tabs)),
        out_shape=(sds((live, width), BF), sds((width, items), BF)) + grad_shapes,
        in_specs=[VMEM_SPEC] * (5 + tabs),
        out_specs=(VMEM_SPEC,) * (2 + len(grad_shapes)),
        scratch_shapes=[
            pltpu.VMEM((live, 4 * width), BF),
            pltpu.VMEM((live, 4 * width), F32),
            pltpu.VMEM((tiles, LANES, LANES), F32),
            pltpu.VMEM((tiles, LANES, LANES), F32),
            pltpu.VMEM((tiles, LANES, LANES), BF),
            pltpu.VMEM((tiles, LANES, LANES), BF),
            pltpu.VMEM((tiles * LANES, LANES), BF),
            pltpu.VMEM((tiles * LANES, LANES), BF),
            pltpu.VMEM((LANES, tiles * LANES), BF),
            pltpu.VMEM((live, width), F32),
            pltpu.VMEM((live, 4 * width), BF),
            pltpu.VMEM((width, live), BF),
            pltpu.VMEM((width, live), BF),
        ],
        compiler_params=pltpu.CompilerParams(vmem_limit_bytes=32 << 20),
        name="layer",
    )(start, onehot, outg, gg, w_near, *pieces)

    def finish_output(gated):
        return pl.pallas_call(
            out_kernel,
            out_shape=sds((rows, width), BF),
            in_specs=[VMEM_SPEC] * 5,
            out_specs=VMEM_SPEC,
            compiler_params=pltpu.CompilerParams(vmem_limit_bytes=16 << 20),
        name="out",
        )(origin, ids2, tab_t, gated, w_out)

    if not halving:
        grad_o, grad_u, grad_t = grads
        grad_t = grad_t.reshape(tabs, feats, dps, span).transpose(2, 0, 1, 3).reshape(devices, feats * span)

        def share(v):
            v = lax.psum_scatter(v, "dp", scatter_dimension=0, tiled=True)
            return lax.psum_scatter(v, "table", scatter_dimension=0, tiled=True)

        return (finish_output(gated), share(grad_t).astype(F32).reshape(feats, span).T, share(grad_u), share(grad_o))

    def add(keep, got):
        return (keep.astype(F32) + got.astype(F32)).astype(BF)

    def halves(v):
        h = v.shape[0] // 2
        return v[:h], v[h:]

    totals = [add(keep, other(send, 1)) for keep, send in zip(grads[::2], grads[1::2])]
    gated, totals[0] = lax.optimization_barrier((gated, totals[0]))
    output = finish_output(gated)
    for n in range(len(ring)):
        for c in range(colours):
            keep, send = halves(totals[c])
            totals[c] = add(keep, swap(send, order[c][1 + n], tab_bits, dps, tabs))
    last = []
    for total in totals:
        keep, send = halves(total)
        last += [keep, swap(send, tab_bits - 1, tab_bits, dps, tabs)]
    grad_uvqk, grad_out_t, grad_t = pl.pallas_call(
        finish_kernel,
        out_shape=(sds((blk, 4 * width), F32), sds((blk, width), F32), sds((feats, span), F32)),
        in_specs=[VMEM_SPEC] * len(last),
        out_specs=(VMEM_SPEC,) * 3,
        compiler_params=pltpu.CompilerParams(vmem_limit_bytes=8 << 20),
        name="finish",
    )(*last)
    return (output, grad_t.T, grad_uvqk, grad_out_t)


def solution(mesh):
    return jax.shard_map(
        layer,
        mesh=mesh,
        in_specs=(
            P("dp"),
            P(("dp", "table"), None),
            P(None, "table"),
            P(),
            P(),
            P(("dp", "table"), None),
        ),
        out_specs=(
            P(("dp", "table"), None),
            P("dp", "table"),
            P(("dp", "table"), None),
            P(("dp", "table"), None),
        ),
        check_vma=False,
    )
```

```python
import functools
import jax
import jax.numpy as jnp
from jax import lax
from jax.experimental import pallas as pl
from jax.experimental.pallas import tpu as pltpu
from jax.sharding import PartitionSpec as P


DH = 64
MAXLEN = 64
LANES = 128
EPS = 1e-05
BF = jnp.bfloat16
F32 = jnp.float32


def nt(a, b):
    return lax.dot_general(a, b, (((1,), (1,)), ((), ())), preferred_element_type=F32)


def nn(a, b):
    return jnp.dot(a, b, preferred_element_type=F32)


def sigmoid(v):
    return 0.5 * jnp.tanh(0.5 * v) + 0.5


def origin_of(packed, len_ref, histories):
    shift = jnp.zeros_like(packed)
    end = jnp.int32(0)
    for b in range(histories):
        end = end + len_ref[0, b]
        shift = shift + jnp.where(packed >= end, MAXLEN - len_ref[0, b], 0)
    return packed + shift


def start_of(packed, len_ref, histories):
    start = jnp.zeros_like(packed)
    end = jnp.int32(0)
    for b in range(histories):
        end = end + len_ref[0, b]
        start = jnp.where(packed >= end, end, start)
    return start


def prep_kernel(
    orders, shape, len_hbm, ids_ref, cot_hbm, wout_hbm, w_hbm, mine_hbm,
    onehot_ref, outg_ref, gg_ref, start_ref, origin_ref, w_ref, mine_ref, outgt_ref,
    len_ref, cot_ref, wout_ref, tmp_ref, sems,
):
    moves = [
        pltpu.make_async_copy(src, dst, sems.at[n])
        for n, (src, dst) in enumerate(
            ((len_hbm, len_ref), (cot_hbm, cot_ref), (wout_hbm, wout_ref), (w_hbm, w_ref), (mine_hbm, mine_ref))
        )
    ]
    for move in moves:
        move.start()
    histories = len_ref.shape[1]
    live, items = onehot_ref.shape
    rows = ids_ref.shape[1]
    own = lax.axis_index("table")
    ids = ids_ref[pl.ds(own, 1), :].astype(F32)
    moves[0].wait()
    start_ref[...] = start_of(lax.broadcasted_iota(jnp.int32, start_ref.shape, 0), len_ref, histories)
    origin_ref[...] = origin_of(lax.broadcasted_iota(jnp.int32, origin_ref.shape, 1), len_ref, histories)
    packed = lax.broadcasted_iota(jnp.int32, (live, rows), 0)
    take = origin_of(packed, len_ref, histories) == lax.broadcasted_iota(jnp.int32, (live, rows), 1)
    own_id = jnp.sum(jnp.where(take, ids, 0.0), axis=1, keepdims=True).astype(jnp.int32)
    onehot_ref[...] = jnp.where(
        lax.broadcasted_iota(jnp.int32, (live, items), 1) == own_id, 1.0, 0.0
    ).astype(BF)
    moves[1].wait()
    out_grad = nn(jnp.where(take, 1.0, 0.0).astype(BF), cot_ref[...]).astype(BF)
    outg_ref[...] = out_grad
    moves[2].wait()
    gg_ref[...] = nt(out_grad, wout_ref[...]).astype(BF)
    tmp_ref[...] = jnp.transpose(out_grad)
    if orders is None:
        outgt_ref[...] = tmp_ref[...]
    else:
        relative_rows(orders[0], shape, tmp_ref, outgt_ref)
    moves[3].wait()
    moves[4].wait()


def out_kernel(origin_ref, ids_ref, tab_ref, gated_ref, wout_ref, out_ref):
    rows = ids_ref.shape[1]
    live = gated_ref.shape[0]
    items = tab_ref.shape[1]
    own = lax.axis_index("table")
    ids = ids_ref[pl.ds(own, 1), :].astype(F32)
    ids_col = jnp.transpose(jnp.broadcast_to(ids, (LANES, rows))).astype(jnp.int32)
    lane = lax.broadcasted_iota(jnp.int32, (rows, LANES), 1)
    onehot = jnp.concatenate(
        [jnp.where(ids_col == lane + k, 1.0, 0.0).astype(BF) for k in range(0, items, LANES)], axis=1
    )
    put = origin_ref[0:1, :] == lax.broadcasted_iota(jnp.int32, (rows, live), 0)
    gated = nn(jnp.where(put, 1.0, 0.0).astype(BF), gated_ref[...]).astype(BF)
    out_ref[...] = (nt(onehot, tab_ref[...]) + nn(gated, wout_ref[...])).astype(BF)


def row_place(order, rel):
    place = 0
    for bit in order:
        place = place * 2 + ((rel >> bit) & 1)
    return place


def relative_rows(order, shape, src_ref, out_ref):
    dps, tabs = shape
    devices = dps * tabs
    me = lax.axis_index("dp") * tabs + lax.axis_index("table")
    blk = src_ref.shape[0] // devices
    for rel in range(devices):
        at = row_place(order, rel) * blk
        src_at = pl.multiple_of((me ^ rel) * blk, blk)
        out_ref[at : at + blk, :] = src_ref[pl.ds(src_at, blk), :]
    return out_ref[...]


def emit(pair, at, lhs, rhs):
    res = nn(lhs, rhs)
    cols = slice(at, at + rhs.shape[1])
    half = res.shape[0] // len(pair)
    for n, ref in enumerate(pair):
        ref[:, cols] = res[n * half : (n + 1) * half].astype(ref.dtype)


def low_half():
    return lax.broadcasted_iota(jnp.int32, (MAXLEN, LANES), 1) < DH


def stack(v):
    zero = jnp.zeros_like(v)
    return jnp.concatenate([jnp.where(low_half(), v, zero), jnp.where(low_half(), zero, v)], axis=0)


def merge(v):
    return jnp.where(low_half(), v[:MAXLEN], v[MAXLEN:])


def spots_of(live, width):
    pairs = width // LANES
    return [
        (t * pairs + c, t * MAXLEN, max(t - 1, 0) * MAXLEN, c * LANES)
        for t in range(live // MAXLEN)
        for c in range(pairs)
    ]


def front_kernel(orders, shape, n_grads, start_ref, onehot_ref, outgt_ref, gg_ref, w_ref, *refs):
    _, tabs = shape
    pieces, refs = refs[:tabs], refs[tabs:]
    grads, refs = refs[:n_grads], refs[n_grads:]
    (
        gated_ref, tab_ref, act_ref, dact_ref, fac_ref, att_ref, qs_ref, datt_ref, xhat_ref, rstd_ref, pgu_ref,
        normt_ref, sc_ref, attended_ref, lhs_ref,
    ) = refs
    live = onehot_ref.shape[0]
    width = tab_ref.shape[0]
    me_tab = lax.axis_index("table")
    for rel in range(tabs):
        feats = pieces[rel].shape[0]
        at = pl.multiple_of((me_tab ^ rel) * feats, feats)
        tab_ref[pl.ds(at, feats), :] = pieces[rel][...]

    x = nt(onehot_ref[...], tab_ref[...])
    centred = x - jnp.mean(x, axis=1, keepdims=True)
    rstd = lax.rsqrt(jnp.mean(centred * centred, axis=1, keepdims=True) + EPS)
    xhat = centred * rstd
    xhat_ref[...] = xhat
    rstd_ref[...] = jnp.broadcast_to(rstd, rstd_ref.shape)
    normed = xhat.astype(BF)
    for g in (2, 3, 1, 0):
        cols = slice(g * width, (g + 1) * width)
        p = nn(normed, w_ref[:, cols])
        s = sigmoid(p)
        a = p * s
        act_ref[:, cols] = a.astype(BF)
        dact_ref[:, cols] = s + a * (1.0 - s)
    normt_ref[...] = jnp.transpose(normed)

    spots = spots_of(live, width)
    pairs = width // LANES
    for n, r0, w0, lo in spots:
        q = stack(act_ref[r0 : r0 + MAXLEN, 2 * width + lo : 2 * width + lo + LANES])
        qs_ref[n] = q
        sc_ref[n] = nt(q, act_ref[w0 : w0 + LANES, 3 * width + lo : 3 * width + lo + LANES])
    for t in range(live // MAXLEN):
        r0 = t * MAXLEN
        row = r0 + lax.broadcasted_iota(jnp.int32, (MAXLEN, LANES), 0)
        col = max(t - 1, 0) * MAXLEN + lax.broadcasted_iota(jnp.int32, (MAXLEN, LANES), 1)
        seen = (col >= start_ref[r0 : r0 + MAXLEN, :]) & (col <= row)
        mask = jnp.where(seen, 1.0 / MAXLEN, 0.0)
        mask = jnp.concatenate([mask, mask], axis=0)
        slope = mask * DH**-0.5
        for c in range(pairs):
            n = t * pairs + c
            sc = sc_ref[n] * DH**-0.5
            sg = sigmoid(sc)
            si = sc * sg
            att_ref[n * LANES : (n + 1) * LANES, :] = (si * mask).astype(BF)
            fac_ref[n] = (sg + si * (1.0 - sg)) * slope
    for n, r0, w0, lo in spots:
        v = act_ref[w0 : w0 + LANES, width + lo : width + lo + LANES]
        attended_ref[r0 : r0 + MAXLEN, lo : lo + LANES] = merge(nn(att_ref[n * LANES : (n + 1) * LANES, :], v))

    attended = attended_ref[...]
    cen = attended - jnp.mean(attended, axis=1, keepdims=True)
    r = lax.rsqrt(jnp.mean(cen * cen, axis=1, keepdims=True) + EPS)
    yhat = cen * r
    u = act_ref[:, :width].astype(F32)
    gated = (yhat * u).astype(BF)
    gated_ref[...] = gated
    gg = gg_ref[...].astype(F32)
    pg_u = ((gg * yhat).astype(BF).astype(F32) * dact_ref[:, :width]).astype(BF)
    pgu_ref[...] = pg_u
    dy = gg * u
    datt = r * (dy - jnp.mean(dy, axis=1, keepdims=True) - yhat * jnp.mean(dy * yhat, axis=1, keepdims=True))
    datt_ref[...] = datt.astype(BF)

    if orders is None:
        emit(grads[:1], 0, outgt_ref[...], gated)
        emit(grads[1:], 0, normt_ref[...], pg_u)
    else:
        emit(grads, 0, outgt_ref[...], gated)
        emit(grads, width, relative_rows(orders[0], shape, normt_ref, lhs_ref), pg_u)


def mid_kernel(act_ref, dact_ref, fac_ref, att_ref, qs_ref, datt_ref, pg_ref, sc_ref, das_ref, ds_ref, turned_ref):
    live, width = datt_ref.shape
    pairs = width // LANES
    tiles = live // MAXLEN
    spots = spots_of(live, width)
    for n, r0, w0, lo in spots:
        da = stack(datt_ref[r0 : r0 + MAXLEN, lo : lo + LANES])
        das_ref[n] = da
        sc_ref[n] = nt(da, act_ref[w0 : w0 + LANES, width + lo : width + lo + LANES])
    for n in range(tiles * pairs):
        dw = sc_ref[n].astype(BF).astype(F32)
        ds_ref[n * LANES : (n + 1) * LANES, :] = (dw * fac_ref[n]).astype(BF)
    for n, r0, w0, lo in spots:
        k = act_ref[w0 : w0 + LANES, 3 * width + lo : 3 * width + lo + LANES]
        dq = merge(nn(ds_ref[n * LANES : (n + 1) * LANES, :], k)).astype(BF).astype(F32)
        slope = dact_ref[r0 : r0 + MAXLEN, 2 * width + lo : 2 * width + lo + LANES]
        pg_ref[r0 : r0 + MAXLEN, width + lo : width + lo + LANES] = (dq * slope).astype(BF)
    for src_ref, rhs_ref, g in ((att_ref, das_ref, 0), (ds_ref, qs_ref, 2)):
        turned_ref[...] = jnp.transpose(src_ref[...])
        for t in range(tiles):
            off = MAXLEN if t else 0
            for c in range(pairs):
                n = t * pairs + c
                lhs = turned_ref[off : off + MAXLEN, n * LANES : (n + 1) * LANES]
                rhs = rhs_ref[n]
                if t + 1 < tiles:
                    m = n + pairs
                    lhs = jnp.concatenate([lhs, turned_ref[:MAXLEN, m * LANES : (m + 1) * LANES]], axis=1)
                    rhs = jnp.concatenate([rhs, rhs_ref[m]], axis=0)
                at = g * width + c * LANES
                rows = slice(t * MAXLEN, (t + 1) * MAXLEN)
                d = nn(lhs, rhs).astype(BF).astype(F32)
                slope = dact_ref[rows, width + at : width + at + LANES]
                pg_ref[rows, at : at + LANES] = (d * slope).astype(BF)


def back_kernel(
    orders, shape, n_grads, pgu_ref, pg_ref, w_ref, xhat_ref, rstd_ref, outg_ref, normt_ref, onehot_ref, *refs
):
    dps, tabs = shape
    grads, (tmp_ref, lhs_ref) = refs[:n_grads], refs[n_grads:]
    _, width = pgu_ref.shape
    items = onehot_ref.shape[1]
    dn = (nt(pgu_ref[...], w_ref[:, :width]) + nt(pg_ref[...], w_ref[:, width:])).astype(BF).astype(F32)
    xhat = xhat_ref[...]
    dx = dn - jnp.mean(dn, axis=1, keepdims=True) - xhat * jnp.mean(dn * xhat, axis=1, keepdims=True)
    in_grad = (rstd_ref[:, :1] * dx + outg_ref[...].astype(F32)).astype(BF)
    tmp_ref[...] = jnp.transpose(in_grad)
    if orders is None:
        emit(grads[:1], 0, normt_ref[...], pg_ref[...])
        emit(grads[1:], 0, tmp_ref[...], onehot_ref[...])
        return
    emit(grads[:2], 0, relative_rows(orders[1], shape, normt_ref, lhs_ref), pg_ref[:, : 2 * width])
    emit(grads[2:], 0, relative_rows(orders[2], shape, normt_ref, lhs_ref), pg_ref[:, 2 * width :])
    me_dp = lax.axis_index("dp")
    me_tab = lax.axis_index("table")
    feats = width // tabs
    span = items // dps
    blk = width // (dps * tabs)
    half = width // 2
    for rt in range(tabs):
        at = pl.multiple_of((me_tab ^ rt) * feats, feats)
        lhs_ref[rt * feats : (rt + 1) * feats, :] = tmp_ref[pl.ds(at, feats), :]
    for rd in range(dps):
        at = pl.multiple_of((me_dp ^ rd) * span, span)
        res = nn(lhs_ref[...], onehot_ref[:, pl.ds(at, span)]).astype(BF)
        for rt in range(tabs):
            place = row_place(orders[2], rd * tabs + rt) * blk
            dst = grads[2] if place < half else grads[3]
            place = place % half
            for j in range(feats // blk):
                dst[place : place + blk, width + j * span : width + (j + 1) * span] = res[
                    rt * feats + j * blk : rt * feats + (j + 1) * blk, :
                ]


def finish_kernel(*refs):
    grad_u_ref, grad_o_ref, grad_t_ref = refs[-3:]
    blk, width = grad_o_ref.shape
    feats, span = grad_t_ref.shape
    first, second, third = (refs[n][...].astype(F32) + refs[n + 1][...].astype(F32) for n in range(0, 6, 2))
    grad_o_ref[...] = first[:, :width]
    grad_u_ref[:, :width] = first[:, width:]
    grad_u_ref[:, width : 3 * width] = second
    grad_u_ref[:, 3 * width :] = third[:, :width]
    for j in range(feats // blk):
        grad_t_ref[j * blk : (j + 1) * blk, :] = third[:, width + j * span : width + (j + 1) * span]


VMEM_SPEC = pl.BlockSpec(memory_space=pltpu.VMEM)
HBM_SPEC = pl.BlockSpec(memory_space=pltpu.HBM)


def in_hbm(v):
    return pltpu.with_memory_space_constraint(v, pltpu.HBM)


def swap(v, bit, tab_bits, dps, tabs):
    if bit < tab_bits:
        return lax.ppermute(v, "table", [(i, i ^ (1 << bit)) for i in range(tabs)])
    b = bit - tab_bits
    return lax.ppermute(v, "dp", [(i, i ^ (1 << b)) for i in range(dps)])


def layer(ids, lengths, table, w_uvqk, w_out, cotangent):
    tabs = lax.axis_size("table")
    dps = lax.axis_size("dp")
    devices = tabs * dps
    tab_bits = tabs.bit_length() - 1
    bits = devices.bit_length() - 1
    histories = lengths.shape[1]
    rows = histories * MAXLEN
    live = rows * 5 // 8
    items = table.shape[0]
    feats = table.shape[1]
    width = feats * tabs
    ids2 = ids.reshape(tabs, rows)

    sds = jax.ShapeDtypeStruct
    ring = list(range(tab_bits, bits)) + list(range(1, tab_bits - 1))
    colours = 3
    blk = width // devices
    span = items // dps
    halving = blk % 16 == 0 and span == LANES and feats % blk == 0 and feats // blk * span == width
    if halving:
        orders = [[0] + ring[c:] + ring[:c] + [tab_bits - 1] for c in (0, 1, 2)]
        front_grads = (sds((width // 2, 2 * width), BF),) * 2
        back_grads = front_grads * 2
    else:
        orders = None
        front_grads = (sds((width, width), F32),) * 2
        back_grads = (sds((width, 3 * width), F32), sds((width, items), BF))


    def other(v, rel):
        return lax.ppermute(v, "table", [(i, i ^ rel) for i in range(tabs)])

    mine = table.T
    far = {}
    for rel in range(2, tabs, 2):
        far[rel] = other(mine, rel)
    onehot, outg, gg, start, origin, w_near, mine_near, outg_t = pl.pallas_call(
        functools.partial(prep_kernel, orders, (dps, tabs)),
        out_shape=(
            sds((live, items), BF),
            sds((live, width), BF),
            sds((live, width), BF),
            sds((live, LANES), jnp.int32),
            sds((8, live), jnp.int32),
            sds(w_uvqk.shape, BF),
            sds(mine.shape, BF),
            sds((width, live), BF),
        ),
        in_specs=[HBM_SPEC, VMEM_SPEC] + [HBM_SPEC] * 4,
        out_specs=(VMEM_SPEC,) * 8,
        scratch_shapes=[
            pltpu.SMEM(lengths.shape, jnp.int32),
            pltpu.VMEM(cotangent.shape, BF),
            pltpu.VMEM(w_out.shape, BF),
            pltpu.VMEM((width, live), BF),
            pltpu.SemaphoreType.DMA((5,)),
        ],
        compiler_params=pltpu.CompilerParams(vmem_limit_bytes=16 << 20),
        name="prep",
    )(in_hbm(lengths), ids2, *map(in_hbm, (cotangent, w_out, w_uvqk, mine)))
    pieces = [mine_near, other(mine, 1)]
    for rel in range(2, tabs, 2):
        pieces += [far[rel], other(far[rel], 1)]

    spots = live // MAXLEN * (width // LANES)

    def kernel(body, operands, outs, scratch, mib):
        return pl.pallas_call(
            body,
            out_shape=outs,
            in_specs=[VMEM_SPEC] * len(operands),
            out_specs=(VMEM_SPEC,) * len(outs),
            scratch_shapes=scratch,
            compiler_params=pltpu.CompilerParams(vmem_limit_bytes=mib << 20),
        )(*operands)

    outs = kernel(
        functools.partial(front_kernel, orders, (dps, tabs), len(front_grads)),
        (start, onehot, outg_t, gg, w_near, *pieces),
        front_grads
        + (
            sds((live, width), BF),
            sds((width, items), BF),
            sds((live, 4 * width), BF),
            sds((live, 4 * width), F32),
            sds((spots, LANES, LANES), F32),
            sds((spots * LANES, LANES), BF),
            sds((spots, LANES, LANES), BF),
            sds((live, width), BF),
            sds((live, width), F32),
            sds((live, LANES), F32),
            sds((live, width), BF),
            sds((width, live), BF),
        ),
        [
            pltpu.VMEM((spots, LANES, LANES), F32),
            pltpu.VMEM((live, width), F32),
            pltpu.VMEM((width, live), BF),
        ],
        24,
    )
    grads, outs = list(outs[: len(front_grads)]), outs[len(front_grads) :]
    gated, tab_t, act, dact, fac, att, qs, datt, xhat, rstd, pg_u, norm_t = outs
    (pg,) = kernel(
        mid_kernel,
        (act, dact, fac, att, qs, datt),
        (sds((live, 3 * width), BF),),
        [
            pltpu.VMEM((spots, LANES, LANES), F32),
            pltpu.VMEM((spots, LANES, LANES), BF),
            pltpu.VMEM((spots * LANES, LANES), BF),
            pltpu.VMEM((LANES, spots * LANES), BF),
        ],
        16,
    )

    def back(pg):
        return kernel(
            functools.partial(back_kernel, orders, (dps, tabs), len(back_grads)),
            (pg_u, pg, w_near, xhat, rstd, outg, norm_t, onehot),
            back_grads,
            [pltpu.VMEM((width, live), BF)] * 2,
            24,
        )

    def finish_output(gated):
        return pl.pallas_call(
            out_kernel,
            out_shape=sds((rows, width), BF),
            in_specs=[VMEM_SPEC] * 5,
            out_specs=VMEM_SPEC,
            compiler_params=pltpu.CompilerParams(vmem_limit_bytes=16 << 20),
        name="out",
        )(origin, ids2, tab_t, gated, w_out)

    if not halving:
        grad_o, grad_gate = grads
        grad_rest, grad_t = back(pg)
        grad_u = jnp.concatenate([grad_gate, grad_rest], axis=1)
        grad_t = grad_t.reshape(tabs, feats, dps, span).transpose(2, 0, 1, 3).reshape(devices, feats * span)

        def share(v):
            v = lax.psum_scatter(v, "dp", scatter_dimension=0, tiled=True)
            return lax.psum_scatter(v, "table", scatter_dimension=0, tiled=True)

        return (finish_output(gated), share(grad_t).astype(F32).reshape(feats, span).T, share(grad_u), share(grad_o))

    def add(keep, got):
        return (keep.astype(F32) + got.astype(F32)).astype(BF)

    def halves(v):
        h = v.shape[0] // 2
        return v[:h], v[h:]

    def step(total, colour, n):
        keep, send = halves(total) if n else total
        got = swap(send, orders[colour][n], tab_bits, dps, tabs)
        if n == len(orders[colour]) - 1:
            return keep, got
        return add(keep, got)

    first = step(grads, 0, 0)
    rest = back(pg)
    totals = [first, step(rest[:2], 1, 0), step(rest[2:], 2, 0)]
    gated, totals[1] = lax.optimization_barrier((gated, totals[1]))
    output = finish_output(gated)
    for n in range(1, len(orders[0]) - 1):
        totals = [step(totals[c], c, n) for c in range(colours)]
    last = []
    for c in range(colours):
        last += step(totals[c], c, len(orders[0]) - 1)
    grad_uvqk, grad_out_t, grad_t = pl.pallas_call(
        finish_kernel,
        out_shape=(sds((blk, 4 * width), F32), sds((blk, width), F32), sds((feats, span), F32)),
        in_specs=[VMEM_SPEC] * len(last),
        out_specs=(VMEM_SPEC,) * 3,
        compiler_params=pltpu.CompilerParams(vmem_limit_bytes=8 << 20),
        name="finish",
    )(*last)
    return (output, grad_t.T, grad_uvqk, grad_out_t)


def solution(mesh):
    return jax.shard_map(
        layer,
        mesh=mesh,
        in_specs=(
            P("dp"),
            P(("dp", "table"), None),
            P(None, "table"),
            P(),
            P(),
            P(("dp", "table"), None),
        ),
        out_specs=(
            P(("dp", "table"), None),
            P("dp", "table"),
            P(("dp", "table"), None),
            P(("dp", "table"), None),
        ),
        check_vma=False,
    )
```

```python
import functools
import jax
import jax.numpy as jnp
from jax import lax
from jax.experimental import pallas as pl
from jax.experimental.pallas import tpu as pltpu
from jax.sharding import PartitionSpec as P


DH = 64
MAXLEN = 64
LANES = 128
EPS = 1e-05
BF = jnp.bfloat16
F32 = jnp.float32


def nt(a, b):
    return lax.dot_general(a, b, (((1,), (1,)), ((), ())), preferred_element_type=F32)


def nn(a, b):
    return jnp.dot(a, b, preferred_element_type=F32)


def sigmoid(v):
    return 0.5 * jnp.tanh(0.5 * v) + 0.5


def origin_of(packed, len_ref, histories):
    shift = jnp.zeros_like(packed)
    end = jnp.int32(0)
    for b in range(histories):
        end = end + len_ref[0, b]
        shift = shift + jnp.where(packed >= end, MAXLEN - len_ref[0, b], 0)
    return packed + shift


def start_of(packed, len_ref, histories):
    start = jnp.zeros_like(packed)
    end = jnp.int32(0)
    for b in range(histories):
        end = end + len_ref[0, b]
        start = jnp.where(packed >= end, end, start)
    return start


def prep_kernel(
    orders, shape, len_hbm, ids_ref, cot_hbm, wout_hbm, w_hbm, mine_hbm,
    onehot_ref, outg_ref, gg_ref, start_ref, origin_ref, w_ref, mine_ref, outgt_ref,
    len_ref, cot_ref, wout_ref, tmp_ref, sems,
):
    moves = [
        pltpu.make_async_copy(src, dst, sems.at[n])
        for n, (src, dst) in enumerate(
            ((len_hbm, len_ref), (cot_hbm, cot_ref), (wout_hbm, wout_ref), (w_hbm, w_ref), (mine_hbm, mine_ref))
        )
    ]
    for move in moves:
        move.start()
    histories = len_ref.shape[1]
    live, items = onehot_ref.shape
    rows = ids_ref.shape[1]
    own = lax.axis_index("table")
    ids = ids_ref[pl.ds(own, 1), :].astype(F32)
    moves[0].wait()
    start_ref[...] = start_of(lax.broadcasted_iota(jnp.int32, start_ref.shape, 0), len_ref, histories)
    origin_ref[...] = origin_of(lax.broadcasted_iota(jnp.int32, origin_ref.shape, 1), len_ref, histories)
    packed = lax.broadcasted_iota(jnp.int32, (live, rows), 0)
    take = origin_of(packed, len_ref, histories) == lax.broadcasted_iota(jnp.int32, (live, rows), 1)
    own_id = jnp.sum(jnp.where(take, ids, 0.0), axis=1, keepdims=True).astype(jnp.int32)
    onehot_ref[...] = jnp.where(
        lax.broadcasted_iota(jnp.int32, (live, items), 1) == own_id, 1.0, 0.0
    ).astype(BF)
    moves[1].wait()
    out_grad = nn(jnp.where(take, 1.0, 0.0).astype(BF), cot_ref[...]).astype(BF)
    outg_ref[...] = out_grad
    moves[2].wait()
    gg_ref[...] = nt(out_grad, wout_ref[...]).astype(BF)
    tmp_ref[...] = jnp.transpose(out_grad)
    if orders is None:
        outgt_ref[...] = tmp_ref[...]
    else:
        relative_rows(orders[0], shape, tmp_ref, outgt_ref)
    moves[3].wait()
    moves[4].wait()


def out_kernel(origin_ref, ids_ref, tab_ref, gated_ref, wout_ref, out_ref):
    rows = ids_ref.shape[1]
    live = gated_ref.shape[0]
    items = tab_ref.shape[1]
    own = lax.axis_index("table")
    ids = ids_ref[pl.ds(own, 1), :].astype(F32)
    ids_col = jnp.transpose(jnp.broadcast_to(ids, (LANES, rows))).astype(jnp.int32)
    lane = lax.broadcasted_iota(jnp.int32, (rows, LANES), 1)
    onehot = jnp.concatenate(
        [jnp.where(ids_col == lane + k, 1.0, 0.0).astype(BF) for k in range(0, items, LANES)], axis=1
    )
    put = origin_ref[0:1, :] == lax.broadcasted_iota(jnp.int32, (rows, live), 0)
    gated = nn(jnp.where(put, 1.0, 0.0).astype(BF), gated_ref[...]).astype(BF)
    out_ref[...] = (nt(onehot, tab_ref[...]) + nn(gated, wout_ref[...])).astype(BF)


def row_place(order, rel):
    place = 0
    for bit in order:
        place = place * 2 + ((rel >> bit) & 1)
    return place


def relative_rows(order, shape, src_ref, out_ref):
    dps, tabs = shape
    devices = dps * tabs
    me = lax.axis_index("dp") * tabs + lax.axis_index("table")
    blk = src_ref.shape[0] // devices
    for rel in range(devices):
        at = row_place(order, rel) * blk
        src_at = pl.multiple_of((me ^ rel) * blk, blk)
        out_ref[at : at + blk, :] = src_ref[pl.ds(src_at, blk), :]
    return out_ref[...]


def emit(pair, at, lhs, rhs):
    res = nn(lhs, rhs)
    cols = slice(at, at + rhs.shape[1])
    half = res.shape[0] // len(pair)
    for n, ref in enumerate(pair):
        ref[:, cols] = res[n * half : (n + 1) * half].astype(ref.dtype)


def low_half():
    return lax.broadcasted_iota(jnp.int32, (MAXLEN, LANES), 1) < DH


def stack(v):
    zero = jnp.zeros_like(v)
    return jnp.concatenate([jnp.where(low_half(), v, zero), jnp.where(low_half(), zero, v)], axis=0)


def merge(v):
    return jnp.where(low_half(), v[:MAXLEN], v[MAXLEN:])


def spots_of(live, width):
    pairs = width // LANES
    return [
        (t * pairs + c, t * MAXLEN, max(t - 1, 0) * MAXLEN, c * LANES)
        for t in range(live // MAXLEN)
        for c in range(pairs)
    ]


def front_kernel(orders, shape, n_grads, start_ref, onehot_ref, outgt_ref, gg_ref, w_ref, *refs):
    _, tabs = shape
    pieces, refs = refs[:tabs], refs[tabs:]
    grads, refs = refs[:n_grads], refs[n_grads:]
    (
        gated_ref, tab_ref, xhat_ref, rstd_ref, pgu_ref, normt_ref, pg_ref,
        act_ref, dact_ref, fac_ref, att_ref, qs_ref, datt_ref, sc_ref, attended_ref, lhs_ref, das_ref, ds_ref, turned_ref,
    ) = refs
    live = onehot_ref.shape[0]
    width = tab_ref.shape[0]
    me_tab = lax.axis_index("table")
    for rel in range(tabs):
        feats = pieces[rel].shape[0]
        at = pl.multiple_of((me_tab ^ rel) * feats, feats)
        tab_ref[pl.ds(at, feats), :] = pieces[rel][...]

    x = nt(onehot_ref[...], tab_ref[...])
    centred = x - jnp.mean(x, axis=1, keepdims=True)
    rstd = lax.rsqrt(jnp.mean(centred * centred, axis=1, keepdims=True) + EPS)
    xhat = centred * rstd
    xhat_ref[...] = xhat
    rstd_ref[...] = jnp.broadcast_to(rstd, rstd_ref.shape)
    normed = xhat.astype(BF)
    for g in (2, 3, 1, 0):
        cols = slice(g * width, (g + 1) * width)
        p = nn(normed, w_ref[:, cols])
        s = sigmoid(p)
        a = p * s
        act_ref[:, cols] = a.astype(BF)
        dact_ref[:, cols] = s + a * (1.0 - s)
    normt_ref[...] = jnp.transpose(normed)

    spots = spots_of(live, width)
    pairs = width // LANES
    for n, r0, w0, lo in spots:
        q = stack(act_ref[r0 : r0 + MAXLEN, 2 * width + lo : 2 * width + lo + LANES])
        qs_ref[n] = q
        sc_ref[n] = nt(q, act_ref[w0 : w0 + LANES, 3 * width + lo : 3 * width + lo + LANES])
    for t in range(live // MAXLEN):
        r0 = t * MAXLEN
        row = r0 + lax.broadcasted_iota(jnp.int32, (MAXLEN, LANES), 0)
        col = max(t - 1, 0) * MAXLEN + lax.broadcasted_iota(jnp.int32, (MAXLEN, LANES), 1)
        seen = (col >= start_ref[r0 : r0 + MAXLEN, :]) & (col <= row)
        mask = jnp.where(seen, 1.0 / MAXLEN, 0.0)
        mask = jnp.concatenate([mask, mask], axis=0)
        slope = mask * DH**-0.5
        for c in range(pairs):
            n = t * pairs + c
            sc = sc_ref[n] * DH**-0.5
            sg = sigmoid(sc)
            si = sc * sg
            att_ref[n * LANES : (n + 1) * LANES, :] = (si * mask).astype(BF)
            fac_ref[n] = (sg + si * (1.0 - sg)) * slope
    for n, r0, w0, lo in spots:
        v = act_ref[w0 : w0 + LANES, width + lo : width + lo + LANES]
        attended_ref[r0 : r0 + MAXLEN, lo : lo + LANES] = merge(nn(att_ref[n * LANES : (n + 1) * LANES, :], v))

    attended = attended_ref[...]
    cen = attended - jnp.mean(attended, axis=1, keepdims=True)
    r = lax.rsqrt(jnp.mean(cen * cen, axis=1, keepdims=True) + EPS)
    yhat = cen * r
    u = act_ref[:, :width].astype(F32)
    gated = (yhat * u).astype(BF)
    gated_ref[...] = gated
    gg = gg_ref[...].astype(F32)
    pg_u = ((gg * yhat).astype(BF).astype(F32) * dact_ref[:, :width]).astype(BF)
    pgu_ref[...] = pg_u
    dy = gg * u
    datt = r * (dy - jnp.mean(dy, axis=1, keepdims=True) - yhat * jnp.mean(dy * yhat, axis=1, keepdims=True))
    datt_ref[...] = datt.astype(BF)

    if orders is None:
        emit(grads[:1], 0, outgt_ref[...], gated)
        emit(grads[1:], 0, normt_ref[...], pg_u)
    else:
        emit(grads, 0, outgt_ref[...], gated)
        emit(grads, width, relative_rows(orders[0], shape, normt_ref, lhs_ref), pg_u)


    mid_body(act_ref, dact_ref, fac_ref, att_ref, qs_ref, datt_ref, pg_ref, sc_ref, das_ref, ds_ref, turned_ref)


def mid_body(act_ref, dact_ref, fac_ref, att_ref, qs_ref, datt_ref, pg_ref, sc_ref, das_ref, ds_ref, turned_ref):
    live, width = datt_ref.shape
    pairs = width // LANES
    tiles = live // MAXLEN
    spots = spots_of(live, width)
    for n, r0, w0, lo in spots:
        da = stack(datt_ref[r0 : r0 + MAXLEN, lo : lo + LANES])
        das_ref[n] = da
        sc_ref[n] = nt(da, act_ref[w0 : w0 + LANES, width + lo : width + lo + LANES])
    for n in range(tiles * pairs):
        dw = sc_ref[n].astype(BF).astype(F32)
        ds_ref[n * LANES : (n + 1) * LANES, :] = (dw * fac_ref[n]).astype(BF)
    for n, r0, w0, lo in spots:
        k = act_ref[w0 : w0 + LANES, 3 * width + lo : 3 * width + lo + LANES]
        dq = merge(nn(ds_ref[n * LANES : (n + 1) * LANES, :], k)).astype(BF).astype(F32)
        slope = dact_ref[r0 : r0 + MAXLEN, 2 * width + lo : 2 * width + lo + LANES]
        pg_ref[r0 : r0 + MAXLEN, width + lo : width + lo + LANES] = (dq * slope).astype(BF)
    for src_ref, rhs_ref, g in ((att_ref, das_ref, 0), (ds_ref, qs_ref, 2)):
        turned_ref[...] = jnp.transpose(src_ref[...])
        for t in range(tiles):
            off = MAXLEN if t else 0
            for c in range(pairs):
                n = t * pairs + c
                lhs = turned_ref[off : off + MAXLEN, n * LANES : (n + 1) * LANES]
                rhs = rhs_ref[n]
                if t + 1 < tiles:
                    m = n + pairs
                    lhs = jnp.concatenate([lhs, turned_ref[:MAXLEN, m * LANES : (m + 1) * LANES]], axis=1)
                    rhs = jnp.concatenate([rhs, rhs_ref[m]], axis=0)
                at = g * width + c * LANES
                rows = slice(t * MAXLEN, (t + 1) * MAXLEN)
                d = nn(lhs, rhs).astype(BF).astype(F32)
                slope = dact_ref[rows, width + at : width + at + LANES]
                pg_ref[rows, at : at + LANES] = (d * slope).astype(BF)


def back_kernel(
    orders, shape, n_grads, pgu_ref, pg_ref, w_ref, xhat_ref, rstd_ref, outg_ref, normt_ref, onehot_ref, *refs
):
    dps, tabs = shape
    grads, (tmp_ref, lhs_ref) = refs[:n_grads], refs[n_grads:]
    _, width = pgu_ref.shape
    items = onehot_ref.shape[1]
    dn = (nt(pgu_ref[...], w_ref[:, :width]) + nt(pg_ref[...], w_ref[:, width:])).astype(BF).astype(F32)
    xhat = xhat_ref[...]
    dx = dn - jnp.mean(dn, axis=1, keepdims=True) - xhat * jnp.mean(dn * xhat, axis=1, keepdims=True)
    in_grad = (rstd_ref[:, :1] * dx + outg_ref[...].astype(F32)).astype(BF)
    tmp_ref[...] = jnp.transpose(in_grad)
    if orders is None:
        emit(grads[:1], 0, normt_ref[...], pg_ref[...])
        emit(grads[1:], 0, tmp_ref[...], onehot_ref[...])
        return
    emit(grads[:2], 0, relative_rows(orders[1], shape, normt_ref, lhs_ref), pg_ref[:, : 2 * width])
    emit(grads[2:], 0, relative_rows(orders[2], shape, normt_ref, lhs_ref), pg_ref[:, 2 * width :])
    me_dp = lax.axis_index("dp")
    me_tab = lax.axis_index("table")
    feats = width // tabs
    span = items // dps
    blk = width // (dps * tabs)
    half = width // 2
    for rt in range(tabs):
        at = pl.multiple_of((me_tab ^ rt) * feats, feats)
        lhs_ref[rt * feats : (rt + 1) * feats, :] = tmp_ref[pl.ds(at, feats), :]
    for rd in range(dps):
        at = pl.multiple_of((me_dp ^ rd) * span, span)
        res = nn(lhs_ref[...], onehot_ref[:, pl.ds(at, span)]).astype(BF)
        for rt in range(tabs):
            place = row_place(orders[2], rd * tabs + rt) * blk
            dst = grads[2] if place < half else grads[3]
            place = place % half
            for j in range(feats // blk):
                dst[place : place + blk, width + j * span : width + (j + 1) * span] = res[
                    rt * feats + j * blk : rt * feats + (j + 1) * blk, :
                ]


def finish_kernel(*refs):
    grad_u_ref, grad_o_ref, grad_t_ref = refs[-3:]
    blk, width = grad_o_ref.shape
    feats, span = grad_t_ref.shape
    first, second, third = (refs[n][...].astype(F32) + refs[n + 1][...].astype(F32) for n in range(0, 6, 2))
    grad_o_ref[...] = first[:, :width]
    grad_u_ref[:, :width] = first[:, width:]
    grad_u_ref[:, width : 3 * width] = second
    grad_u_ref[:, 3 * width :] = third[:, :width]
    for j in range(feats // blk):
        grad_t_ref[j * blk : (j + 1) * blk, :] = third[:, width + j * span : width + (j + 1) * span]


VMEM_SPEC = pl.BlockSpec(memory_space=pltpu.VMEM)
HBM_SPEC = pl.BlockSpec(memory_space=pltpu.HBM)


def in_hbm(v):
    return pltpu.with_memory_space_constraint(v, pltpu.HBM)


def swap(v, bit, tab_bits, dps, tabs):
    if bit < tab_bits:
        return lax.ppermute(v, "table", [(i, i ^ (1 << bit)) for i in range(tabs)])
    b = bit - tab_bits
    return lax.ppermute(v, "dp", [(i, i ^ (1 << b)) for i in range(dps)])


def layer(ids, lengths, table, w_uvqk, w_out, cotangent):
    tabs = lax.axis_size("table")
    dps = lax.axis_size("dp")
    devices = tabs * dps
    tab_bits = tabs.bit_length() - 1
    bits = devices.bit_length() - 1
    histories = lengths.shape[1]
    rows = histories * MAXLEN
    live = rows * 5 // 8
    items = table.shape[0]
    feats = table.shape[1]
    width = feats * tabs
    ids2 = ids.reshape(tabs, rows)

    sds = jax.ShapeDtypeStruct
    ring = list(range(tab_bits, bits)) + list(range(1, tab_bits - 1))
    colours = 3
    blk = width // devices
    span = items // dps
    halving = blk % 16 == 0 and span == LANES and feats % blk == 0 and feats // blk * span == width
    if halving:
        orders = [[0] + ring[c:] + ring[:c] + [tab_bits - 1] for c in (0, 1, 2)]
        front_grads = (sds((width // 2, 2 * width), BF),) * 2
        back_grads = front_grads * 2
    else:
        orders = None
        front_grads = (sds((width, width), F32),) * 2
        back_grads = (sds((width, 3 * width), F32), sds((width, items), BF))


    def other(v, rel):
        return lax.ppermute(v, "table", [(i, i ^ rel) for i in range(tabs)])

    mine = table.T
    far = {}
    for rel in range(2, tabs, 2):
        far[rel] = other(mine, rel)
    onehot, outg, gg, start, origin, w_near, mine_near, outg_t = pl.pallas_call(
        functools.partial(prep_kernel, orders, (dps, tabs)),
        out_shape=(
            sds((live, items), BF),
            sds((live, width), BF),
            sds((live, width), BF),
            sds((live, LANES), jnp.int32),
            sds((8, live), jnp.int32),
            sds(w_uvqk.shape, BF),
            sds(mine.shape, BF),
            sds((width, live), BF),
        ),
        in_specs=[HBM_SPEC, VMEM_SPEC] + [HBM_SPEC] * 4,
        out_specs=(VMEM_SPEC,) * 8,
        scratch_shapes=[
            pltpu.SMEM(lengths.shape, jnp.int32),
            pltpu.VMEM(cotangent.shape, BF),
            pltpu.VMEM(w_out.shape, BF),
            pltpu.VMEM((width, live), BF),
            pltpu.SemaphoreType.DMA((5,)),
        ],
        compiler_params=pltpu.CompilerParams(vmem_limit_bytes=16 << 20),
        name="prep",
    )(in_hbm(lengths), ids2, *map(in_hbm, (cotangent, w_out, w_uvqk, mine)))
    pieces = [mine_near, other(mine, 1)]
    for rel in range(2, tabs, 2):
        pieces += [far[rel], other(far[rel], 1)]

    spots = live // MAXLEN * (width // LANES)

    def kernel(body, operands, outs, scratch, mib):
        return pl.pallas_call(
            body,
            out_shape=outs,
            in_specs=[VMEM_SPEC] * len(operands),
            out_specs=(VMEM_SPEC,) * len(outs),
            scratch_shapes=scratch,
            compiler_params=pltpu.CompilerParams(vmem_limit_bytes=mib << 20),
        )(*operands)

    outs = kernel(
        functools.partial(front_kernel, orders, (dps, tabs), len(front_grads)),
        (start, onehot, outg_t, gg, w_near, *pieces),
        front_grads
        + (
            sds((live, width), BF),
            sds((width, items), BF),
            sds((live, width), F32),
            sds((live, LANES), F32),
            sds((live, width), BF),
            sds((width, live), BF),
            sds((live, 3 * width), BF),
        ),
        [
            pltpu.VMEM((live, 4 * width), BF),
            pltpu.VMEM((live, 4 * width), F32),
            pltpu.VMEM((spots, LANES, LANES), F32),
            pltpu.VMEM((spots * LANES, LANES), BF),
            pltpu.VMEM((spots, LANES, LANES), BF),
            pltpu.VMEM((live, width), BF),
            pltpu.VMEM((spots, LANES, LANES), F32),
            pltpu.VMEM((live, width), F32),
            pltpu.VMEM((width, live), BF),
            pltpu.VMEM((spots, LANES, LANES), BF),
            pltpu.VMEM((spots * LANES, LANES), BF),
            pltpu.VMEM((LANES, spots * LANES), BF),
        ],
        28,
    )
    grads, outs = list(outs[: len(front_grads)]), outs[len(front_grads) :]
    gated, tab_t, xhat, rstd, pg_u, norm_t, pg = outs

    def back(pg):
        return kernel(
            functools.partial(back_kernel, orders, (dps, tabs), len(back_grads)),
            (pg_u, pg, w_near, xhat, rstd, outg, norm_t, onehot),
            back_grads,
            [pltpu.VMEM((width, live), BF)] * 2,
            24,
        )

    def finish_output(gated):
        return pl.pallas_call(
            out_kernel,
            out_shape=sds((rows, width), BF),
            in_specs=[VMEM_SPEC] * 5,
            out_specs=VMEM_SPEC,
            compiler_params=pltpu.CompilerParams(vmem_limit_bytes=16 << 20),
        name="out",
        )(origin, ids2, tab_t, gated, w_out)

    if not halving:
        grad_o, grad_gate = grads
        grad_rest, grad_t = back(pg)
        grad_u = jnp.concatenate([grad_gate, grad_rest], axis=1)
        grad_t = grad_t.reshape(tabs, feats, dps, span).transpose(2, 0, 1, 3).reshape(devices, feats * span)

        def share(v):
            v = lax.psum_scatter(v, "dp", scatter_dimension=0, tiled=True)
            return lax.psum_scatter(v, "table", scatter_dimension=0, tiled=True)

        return (finish_output(gated), share(grad_t).astype(F32).reshape(feats, span).T, share(grad_u), share(grad_o))

    def add(keep, got):
        return (keep.astype(F32) + got.astype(F32)).astype(BF)

    def halves(v):
        h = v.shape[0] // 2
        return v[:h], v[h:]

    def step(total, colour, n):
        keep, send = halves(total) if n else total
        got = swap(send, orders[colour][n], tab_bits, dps, tabs)
        if n == len(orders[colour]) - 1:
            return keep, got
        return add(keep, got)

    first = step(grads, 0, 0)
    rest = back(pg)
    totals = [first, step(rest[:2], 1, 0), step(rest[2:], 2, 0)]
    gated, totals[1] = lax.optimization_barrier((gated, totals[1]))
    output = finish_output(gated)
    for n in range(1, len(orders[0]) - 1):
        totals = [step(totals[c], c, n) for c in range(colours)]
    last = []
    for c in range(colours):
        last += step(totals[c], c, len(orders[0]) - 1)
    grad_uvqk, grad_out_t, grad_t = pl.pallas_call(
        finish_kernel,
        out_shape=(sds((blk, 4 * width), F32), sds((blk, width), F32), sds((feats, span), F32)),
        in_specs=[VMEM_SPEC] * len(last),
        out_specs=(VMEM_SPEC,) * 3,
        compiler_params=pltpu.CompilerParams(vmem_limit_bytes=8 << 20),
        name="finish",
    )(*last)
    return (output, grad_t.T, grad_uvqk, grad_out_t)


def solution(mesh):
    return jax.shard_map(
        layer,
        mesh=mesh,
        in_specs=(
            P("dp"),
            P(("dp", "table"), None),
            P(None, "table"),
            P(),
            P(),
            P(("dp", "table"), None),
        ),
        out_specs=(
            P(("dp", "table"), None),
            P("dp", "table"),
            P(("dp", "table"), None),
            P(("dp", "table"), None),
        ),
        check_vma=False,
    )
```
